32 devices in a mesh: row: 2 (over x), col: 4 (over y, core), dp: 4 (over z).
Axes of the slice: x: 2, y: 2, z: 4, core: 2. Of those that a mesh axis runs over, the one named last changes fastest.
Arguments:
- latents: bfloat16 [4, 1024, 1024], P('dp', 'col', 'row'), may hold values from -6 to 6
- inputs: bfloat16 [4, 8192, 261], P('dp', 'col'), may hold values from -6 to 6
- positions: int32 [4, 1024], P('dp'), may hold values from 0 to 8191, as said below
- piece_start: int32 [4, 8], P('dp'), may hold values from 0 to 7936, as said below
- cotangent: bfloat16 [4, 1024, 1024], P('dp', 'col', 'row'), may hold values from -6 to 6
- cross_gain: float32 [1024], P('row'), may hold values from 0.25 to 1.75
- input_gain: float32 [261], replicated, may hold values from 0.25 to 1.75
- cross_query: bfloat16 [1024, 1024], P('row', 'col'), may hold values from -0.1875 to 0.1875
- cross_key: bfloat16 [261, 1024], replicated, may hold values from -0.375 to 0.375
- cross_value: bfloat16 [261, 1024], replicated, may hold values from -0.375 to 0.375
- cross_out: bfloat16 [1024, 1024], P('col', 'row'), may hold values from -4 to 4
- first_gain: float32 [1024], P('row'), may hold values from 0.25 to 1.75
- first_expand: bfloat16 [1024, 1024], P('row', 'col'), may hold values from -0.1875 to 0.1875
- first_shrink: bfloat16 [1024, 1024], P('col', 'row'), may hold values from -0.1875 to 0.1875
- self_gain: float32 [1024], P('row'), may hold values from 0.25 to 1.75
- self_query: bfloat16 [1024, 1024], P('row', 'col'), may hold values from -0.1875 to 0.1875
- self_key: bfloat16 [1024, 1024], P('row', 'col'), may hold values from -0.1875 to 0.1875
- self_value: bfloat16 [1024, 1024], P('row', 'col'), may hold values from -0.1875 to 0.1875
- self_out: bfloat16 [1024, 1024], P('col', 'row'), may hold values from -2 to 2
- second_gain: float32 [1024], P('row'), may hold values from 0.25 to 1.75
- second_expand: bfloat16 [1024, 1024], P('row', 'col'), may hold values from -0.1875 to 0.1875
- second_shrink: bfloat16 [1024, 1024], P('col', 'row'), may hold values from -0.1875 to 0.1875
Outputs:
- out: bfloat16 [4, 1024, 1024], P('dp', 'col', 'row')
- grad_latents: float32 [4, 1024, 1024], P('dp', 'col', 'row')
- grad_inputs: bfloat16 [4, 8192, 261], P('dp', 'col')
- grad_cross_gain: float32 [1024], P('row')
- grad_input_gain: float32 [261], replicated
- grad_cross_query: float32 [1024, 1024], P('row', 'col')
- grad_cross_key: float32 [261, 1024], replicated
- grad_cross_value: float32 [261, 1024], replicated
- grad_cross_out: float32 [1024, 1024], P('col', 'row')
- grad_first_gain: float32 [1024], P('row')
- grad_first_expand: float32 [1024, 1024], P('row', 'col')
- grad_first_shrink: float32 [1024, 1024], P('col', 'row')
- grad_self_gain: float32 [1024], P('row')
- grad_self_query: float32 [1024, 1024], P('row', 'col')
- grad_self_key: float32 [1024, 1024], P('row', 'col')
- grad_self_value: float32 [1024, 1024], P('row', 'col')
- grad_self_out: float32 [1024, 1024], P('col', 'row')
- grad_second_gain: float32 [1024], P('row')
- grad_second_expand: float32 [1024, 1024], P('row', 'col')
- grad_second_shrink: float32 [1024, 1024], P('col', 'row')
The draws below stay inside these ranges and needn't reach their ends.
Inputs may be any that keep to these rules, and one draw needn't show every extreme that they name: `positions`: latent i of a sequence stands in rows i * 8 to (i + 1) * 8 - 1. `piece_start`: piece p starts in the slot of rows from p * 1024 and its 256 rows end within that slot.
All inputs are finite; a program needn't handle non-finite values.
Results may differ from the reference program's by a relative error of at most 0.04.
Values may be sent and summed in bfloat16 or wider, within the bound.
No kernel may reach another device: no remote copies, remote signals or barrier semaphores. Data moves between devices by JAX's collectives and lax.ppermute only.
A program may use at most 128 MiB of HBM per device.

```python
import math
import jax
import jax.numpy as jnp
from jax import lax

D = 1024
CIN = 261
HEADS = 8
HEAD = 128
S_LEN = 8192
LAT_SEQ = 1024
PIECES = 8
PIECE_LEN = 256
SEQS = 4


def draw_positions(key, part):
    stride = S_LEN // LAT_SEQ
    offsets = jax.random.randint(key, (SEQS, LAT_SEQ), 0, stride, dtype=jnp.int32)
    return jnp.arange(LAT_SEQ, dtype=jnp.int32)[None, :] * stride + offsets


def draw_piece_start(key, part):
    slot = S_LEN // PIECES
    offsets = jax.random.randint(key, (SEQS, PIECES), 0, slot - PIECE_LEN + 1, dtype=jnp.int32)
    return jnp.arange(PIECES, dtype=jnp.int32)[None, :] * slot + offsets


def block_levels(key, extent, pieces, low, top_value):
    level = 1.0
    for position, blocks in pieces:
        draws = jax.random.uniform(jax.random.fold_in(jax.random.fold_in(key, 6), position), (blocks,), jnp.float32, low / len(pieces), top_value / len(pieces))
        level = level * jnp.repeat(jnp.exp(draws), extent[position] // blocks).reshape((-1,) + (1,) * (len(extent) - 1 - position))
    return level


def centred(stream_key, extent, scale, most, shards=(), kind=jnp.bfloat16):
    array = jax.random.normal(stream_key, extent, jnp.float32) * scale
    if len(shards) > 0:
        array = block_levels(stream_key, extent, shards, -0.22, 0.18) * array
    return jnp.clip(array, min=-most, max=most).astype(kind)


def setup_inputs(seed: int = 0) -> dict:
    key_of = jax.random.split(jax.random.key(seed), 23)
    return {
        "latents": centred(key_of[0], (SEQS, LAT_SEQ, D), 1.0, 6.0, ((0, 4), (1, 4), (2, 2))),
        "inputs": centred(key_of[1], (SEQS, S_LEN, CIN), 1.0, 6.0, ((0, 4), (1, 4))),
        "positions": draw_positions(jax.random.fold_in(key_of[22], 71), 0),
        "piece_start": draw_piece_start(jax.random.fold_in(key_of[22], 71), 0),
        "cotangent": centred(key_of[4], (SEQS, LAT_SEQ, D), 1.0, 6.0, ((0, 4), (1, 4), (2, 2))),
        "cross_gain": jnp.clip(1.0 + 0.15 * jax.random.normal(key_of[5], (D,), jnp.float32), 0.25, 1.75),
        "input_gain": jnp.clip(1.0 + 0.15 * jax.random.normal(key_of[6], (CIN,), jnp.float32), 0.25, 1.75),
        "cross_query": centred(key_of[7], (D, D), D ** -0.5, 0.1875, ((0, 2), (1, 4))),
        "cross_key": centred(key_of[8], (CIN, D), CIN ** -0.5, 0.375),
        "cross_value": centred(key_of[9], (CIN, D), CIN ** -0.5, 0.375),
        "cross_out": centred(key_of[10], (D, D), (max(D // 512, 1)) ** -0.5, 4.0, ((0, 4), (1, 2))),
        "first_gain": jnp.clip(1.0 + 0.15 * jax.random.normal(key_of[11], (D,), jnp.float32), 0.25, 1.75),
        "first_expand": centred(key_of[12], (D, D), D ** -0.5, 0.1875, ((0, 2), (1, 4))),
        "first_shrink": centred(key_of[13], (D, D), D ** -0.5, 0.1875, ((0, 4), (1, 2))),
        "self_gain": jnp.clip(1.0 + 0.15 * jax.random.normal(key_of[14], (D,), jnp.float32), 0.25, 1.75),
        "self_query": centred(key_of[15], (D, D), D ** -0.5, 0.1875, ((0, 2), (1, 4))),
        "self_key": centred(key_of[16], (D, D), D ** -0.5, 0.1875, ((0, 2), (1, 4))),
        "self_value": centred(key_of[17], (D, D), D ** -0.5, 0.1875, ((0, 2), (1, 4))),
        "self_out": centred(key_of[18], (D, D), (max(D // 128, 1)) ** -0.5, 2.0, ((0, 4), (1, 2))),
        "second_gain": jnp.clip(1.0 + 0.15 * jax.random.normal(key_of[19], (D,), jnp.float32), 0.25, 1.75),
        "second_expand": centred(key_of[20], (D, D), D ** -0.5, 0.1875, ((0, 2), (1, 4))),
        "second_shrink": centred(key_of[21], (D, D), D ** -0.5, 0.1875, ((0, 4), (1, 2))),
    }


EPS = 1e-05
NEGATIVE = -1e+30

@jax.custom_vjp
def low(v):
    return lax.optimization_barrier(v.astype(jnp.bfloat16)).astype(jnp.float32)

@jax.custom_vjp
def low_back(v):
    return v

def low_keep(v):
    return (low(v), None)

def low_pass(kept, grad):
    return (grad,)

def back_keep(v):
    return (v, None)

def back_low(kept, grad):
    return (low(grad),)
low.defvjp(low_keep, low_pass)
low_back.defvjp(back_keep, back_low)

def rounded_both(value):
    return low_back(low(value))

def matmul(left, right):
    return jnp.dot(left, right, precision=lax.Precision.HIGHEST, preferred_element_type=jnp.float32)

def norm(value, gain):
    center = lax.optimization_barrier(jnp.mean(value, axis=-1, keepdims=True))
    shifted = value - center
    spread = lax.optimization_barrier(jnp.mean(shifted * shifted, axis=-1, keepdims=True))
    return shifted * lax.rsqrt(spread + EPS) * gain

def gelu_exact(value):
    return jax.nn.gelu(value, approximate=False)

def view_limits(positions, starts):
    ends = starts + PIECE_LEN
    inside = (starts[:, None, :] <= positions[:, :, None]) & (positions[:, :, None] < ends[:, None, :])
    reach = lax.optimization_barrier(jnp.sum(jnp.where(inside, ends[:, None, :], 0), axis=-1)).astype(jnp.int32)
    return jnp.maximum(positions + 1, reach).astype(jnp.int32)

def feed(state, gain, expand, shrink):
    hidden = low(norm(state, gain))
    upward = low_back(matmul(hidden, expand))
    active = low(gelu_exact(upward))
    return low_back(matmul(active, shrink))

def one_sequence(state, rows, limit, places, weights):
    cross_gain, input_gain, cross_query, cross_key, cross_value, cross_out, first_gain, first_expand, first_shrink, self_gain, self_query, self_key, self_value, self_out, second_gain, second_expand, second_shrink = weights
    cross_in = low(norm(state, cross_gain))
    input_in = low(norm(rows, input_gain))
    query = rounded_both(matmul(cross_in, cross_query))
    keys = low(matmul(input_in, cross_key))
    values = low(matmul(input_in, cross_value))
    scores = low_back(matmul(query, keys.T) * (1.0 / math.sqrt(D)))
    mask = jnp.arange(S_LEN, dtype=jnp.int32)[None, :] < limit[:, None]
    chances = low(jax.nn.softmax(jnp.where(mask, scores, NEGATIVE), axis=-1))
    attended = rounded_both(matmul(chances, values))
    after_cross = state + low_back(matmul(attended, cross_out))
    after_first = after_cross + feed(after_cross, first_gain, first_expand, first_shrink)
    self_in = low(norm(after_first, self_gain))
    heads_q = rounded_both(matmul(self_in, self_query)).reshape(LAT_SEQ, HEADS, HEAD)
    heads_k = rounded_both(matmul(self_in, self_key)).reshape(LAT_SEQ, HEADS, HEAD)
    heads_v = rounded_both(matmul(self_in, self_value)).reshape(LAT_SEQ, HEADS, HEAD)
    self_scores = jnp.einsum('qhd,khd->hqk', heads_q, heads_k, precision=lax.Precision.HIGHEST, preferred_element_type=jnp.float32) * (1.0 / math.sqrt(HEAD))
    self_scores = low_back(self_scores)
    latent_attend_mask = places[None, :] < limit[:, None]
    self_chances = low(jax.nn.softmax(jnp.where(latent_attend_mask[None], self_scores, NEGATIVE), axis=-1))
    mixed = jnp.einsum('hqk,khd->qhd', self_chances, heads_v, precision=lax.Precision.HIGHEST, preferred_element_type=jnp.float32).reshape(LAT_SEQ, D)
    mixed = rounded_both(mixed)
    after_self = after_first + low_back(matmul(mixed, self_out))
    return after_self + feed(after_self, second_gain, second_expand, second_shrink)

def reference(latents, inputs, positions, piece_start, cotangent, cross_gain, input_gain, cross_query, cross_key, cross_value, cross_out, first_gain, first_expand, first_shrink, self_gain, self_query, self_key, self_value, self_out, second_gain, second_expand, second_shrink):
    limits = view_limits(positions, piece_start)
    params = tuple((item.astype(jnp.float32) for item in (cross_gain, input_gain, cross_query, cross_key, cross_value, cross_out, first_gain, first_expand, first_shrink, self_gain, self_query, self_key, self_value, self_out, second_gain, second_expand, second_shrink)))

    def forward(states, rows, *weights):

        def step(item):
            return one_sequence(item[0], item[1], item[2], item[3], weights)
        return lax.map(jax.checkpoint(step), (states, rows, limits, positions))
    result, pull = jax.vjp(forward, latents.astype(jnp.float32), inputs.astype(jnp.float32), *params)
    grads = pull(cotangent.astype(jnp.float32))
    return (result.astype(jnp.bfloat16), grads[0], grads[1].astype(jnp.bfloat16), grads[2], grads[3], grads[4], grads[5], grads[6], grads[7], grads[8], grads[9], grads[10], grads[11], grads[12], grads[13], grads[14], grads[15], grads[16], grads[17], grads[18])
```

```python
import functools
import math

import jax
import jax.numpy as jnp
from jax import lax
from jax.experimental import pallas as pl
from jax.experimental.pallas import tpu as pltpu
from jax.sharding import PartitionSpec as P

D = 1024
HEAD = 128
PIECE_LEN = 256


EPS = 1e-05
NEGATIVE = -1e30
FORWARD_FIRST = "xok,kt->xot"
BACKWARD_FIRST = "tpv,qv->tpq"
FORWARD_SECOND = "ybj,jv->ybv"
BACKWARD_SECOND = "xng,wg->xnw"
GRADIENT_FIRST = "zyq,zyi->qi"
GRADIENT_SECOND = "oqv,oqa->va"


def joined_2(shard, axis, combine):
    everything = jax.tree.map(lambda part: lax.all_gather(part, axis), shard)
    first = jax.tree.map(lambda part: part[0], everything)

    def step(k, so_far):
        return combine(so_far, jax.tree.map(lambda part: part[k], everything))

    return lax.fori_loop(1, lax.axis_size(axis), step, first)


def col_rows(value):
    return lax.all_gather(value, "col", axis=1, tiled=True)


def row_reduce(value):
    return lax.psum_scatter(
        value.astype(jnp.bfloat16), "row", scatter_dimension=1, tiled=True
    ).astype(jnp.float32)


def row_rows(value):
    return lax.all_gather(value, "row", axis=1, tiled=True)


def col_reduce(value):
    return lax.psum_scatter(
        value.astype(jnp.bfloat16), "col", scatter_dimension=1, tiled=True
    ).astype(jnp.float32)


def query_feats(value):
    return lax.all_gather(value, "col", axis=2, tiled=True)


def query_grads(value):
    return lax.psum_scatter(
        value.astype(jnp.bfloat16), "col", scatter_dimension=2, tiled=True
    ).astype(jnp.float32)


def row_totals(first, second):
    return lax.psum((first, second), "row")


def project_cols(value, weight, form):
    gathered = col_rows(value)
    partial_sum = jnp.einsum(form, gathered, weight, preferred_element_type=jnp.float32)
    return (row_reduce(partial_sum), gathered)


def project_rows(value, weight, form):
    gathered = row_rows(value)
    partial_sum = jnp.einsum(form, gathered, weight, preferred_element_type=jnp.float32)
    return (col_reduce(partial_sum), gathered)


def weight_grad(form, first, second):
    return jnp.einsum(form, first, second, preferred_element_type=jnp.float32)


def split_parts(value):
    leading = value.astype(jnp.bfloat16)
    residue = (value - leading.astype(jnp.float32)).astype(jnp.bfloat16)
    return (leading, residue)


def split_einsum(form, exact, other, first_side):
    leading, residue = split_parts(exact)
    if first_side:
        return jnp.einsum(form, leading, other, preferred_element_type=jnp.float32) + jnp.einsum(
            form, residue, other, preferred_element_type=jnp.float32
        )
    return jnp.einsum(form, other, leading, preferred_element_type=jnp.float32) + jnp.einsum(
        form, other, residue, preferred_element_type=jnp.float32
    )


def norm_forward(value, gain):
    width = value.shape[-1] * lax.axis_size("row")
    total, squares = row_totals(jnp.sum(value, axis=-1), jnp.sum(value * value, axis=-1))
    center = total / width
    spread = squares / width - center * center
    scale_inv = lax.rsqrt(spread + EPS)
    normed = (value - center[..., None]) * scale_inv[..., None]
    return (normed * gain, normed, scale_inv)


def norm_backward(grad, gain, normed, scale_inv):
    width = grad.shape[-1] * lax.axis_size("row")
    scaled = grad * gain
    first, second = row_totals(jnp.sum(scaled, axis=-1), jnp.sum(scaled * normed, axis=-1))
    result = scale_inv[..., None] * (
        scaled - first[..., None] / width - normed * (second[..., None] / width)
    )
    return (result, jnp.sum(grad * normed, axis=(0, 1)))


def gelu_exact(value):
    return jax.nn.gelu(value, approximate=False)


def gelu_back(value, grad):
    return jax.vjp(gelu_exact, value)[1](grad)[0]


def view_limits(positions, starts):
    ends = starts + PIECE_LEN
    inside = (starts[:, None, :] <= positions[:, :, None]) & (
        positions[:, :, None] < ends[:, None, :]
    )
    reach = jnp.sum(jnp.where(inside, ends[:, None, :], 0), axis=-1)
    return jnp.maximum(positions + 1, reach)


def merge_softmax(first, second):
    top = jnp.maximum(first[0], second[0])
    return (top, first[1] * jnp.exp(first[0] - top) + second[1] * jnp.exp(second[0] - top))


def feed_forward(state, gain, expand, shrink):
    normed_out, normed, scale_inv = norm_forward(state, gain)
    upward, hidden_rows = project_cols(normed_out.astype(jnp.bfloat16), expand, FORWARD_FIRST)
    activated = gelu_exact(upward).astype(jnp.bfloat16)
    branch, active_rows = project_rows(activated, shrink, FORWARD_SECOND)
    return (state + branch, (normed, scale_inv, hidden_rows, upward, active_rows))


def feed_backward(grad, saved, gain, expand, shrink):
    normed, scale_inv, hidden_rows, upward, active_rows = saved
    grad_active, branch_rows = project_cols(grad.astype(jnp.bfloat16), shrink, BACKWARD_SECOND)
    grad_shrink = weight_grad(GRADIENT_SECOND, active_rows, branch_rows)
    grad_upward = gelu_back(upward, grad_active).astype(jnp.bfloat16)
    grad_hidden, upward_rows = project_rows(grad_upward, expand, BACKWARD_FIRST)
    grad_expand = weight_grad(GRADIENT_FIRST, hidden_rows, upward_rows)
    grad_normed, grad_gain = norm_backward(grad_hidden, gain, normed, scale_inv)
    return (grad + grad_normed, grad_gain, grad_expand, grad_shrink)


def input_back(grad_part, normed, scale_inv, gain):
    scaled = grad_part * gain
    first = jnp.mean(scaled, axis=-1, keepdims=True)
    second = jnp.mean(scaled * normed, axis=-1, keepdims=True)
    return scale_inv[..., None] * (scaled - first - normed * second)


def on_device(
    latents,
    inputs,
    positions,
    piece_start,
    cotangent,
    cross_gain,
    input_gain,
    cross_query,
    cross_key,
    cross_value,
    cross_out,
    first_gain,
    first_expand,
    first_shrink,
    self_gain,
    self_query,
    self_key,
    self_value,
    self_out,
    second_gain,
    second_expand,
    second_shrink,
):
    low_type = jnp.bfloat16
    full_type = jnp.float32
    row_at = lax.axis_index("row")
    col_at = lax.axis_index("col")
    seqs = latents.shape[0]
    total_rows = positions.shape[1]
    rows_here = total_rows // lax.axis_size("row")
    column_width_count = cross_query.shape[1]
    width_row = cross_query.shape[0]
    key_rows = inputs.shape[1]
    heads_here = column_width_count // HEAD
    cross_scale = 1.0 / math.sqrt(D)
    self_scale = 1.0 / math.sqrt(HEAD)
    limit_all = view_limits(positions, piece_start)
    limit_here = lax.dynamic_slice_in_dim(limit_all, row_at * rows_here, rows_here, 1)
    key_index = col_at * key_rows + jnp.arange(key_rows, dtype=jnp.int32)
    cross_mask = key_index[None, None, :] < limit_here[:, :, None]
    latent_attend_mask = (positions[:, None, :] < limit_here[:, :, None])[:, None]
    initial = latents.astype(full_type)
    cross_normed_out, cross_normed, cross_inv = norm_forward(initial, cross_gain)
    query_part, cross_rows = project_cols(
        cross_normed_out.astype(low_type), cross_query, FORWARD_FIRST
    )
    query_all = query_feats(query_part.astype(low_type))
    input_full = inputs.astype(full_type)
    input_center = input_full - jnp.mean(input_full, axis=-1, keepdims=True)
    input_inv = lax.rsqrt(jnp.mean(input_center * input_center, axis=-1) + EPS)
    input_normed = input_center * input_inv[..., None]
    input_low = (input_normed * input_gain).astype(low_type)

    def project_keys(rows):
        key_block = jnp.dot(rows, cross_key, preferred_element_type=full_type).astype(low_type)
        value_block = jnp.dot(rows, cross_value, preferred_element_type=full_type).astype(low_type)
        return (key_block, value_block)

    keys_all, values_all = lax.map(project_keys, input_low)
    scores = (
        jnp.einsum("sqd,skd->sqk", query_all, keys_all, preferred_element_type=full_type)
        * cross_scale
    )
    local_top = jnp.max(jnp.where(cross_mask, scores, NEGATIVE), axis=-1)
    local_total = jnp.sum(
        jnp.where(cross_mask, jnp.exp(scores - local_top[..., None]), 0.0), axis=-1
    )
    merged_top, merged_total = joined_2((local_top, local_total), "col", merge_softmax)
    cross_lse = merged_top + jnp.log(merged_total)
    cross_chances = jnp.where(cross_mask, jnp.exp(scores - cross_lse[..., None]), 0.0).astype(
        low_type
    )
    attended_part = jnp.einsum(
        "sqk,skd->sqd", cross_chances, values_all, preferred_element_type=full_type
    )
    attended_all = lax.psum(attended_part.astype(jnp.bfloat16), "col").astype(jnp.float32)
    attended_here = lax.dynamic_slice_in_dim(
        attended_all, col_at * column_width_count, column_width_count, 2
    )
    cross_branch, attended_rows = project_rows(
        attended_here.astype(low_type), cross_out, FORWARD_SECOND
    )
    after_cross = initial + cross_branch
    after_first, first_saved = feed_forward(after_cross, first_gain, first_expand, first_shrink)
    self_normed_out, self_normed, self_inv = norm_forward(after_first, self_gain)
    joined = jnp.concatenate([self_query, self_key, self_value], axis=1)
    projected, self_rows = project_cols(self_normed_out.astype(low_type), joined, FORWARD_FIRST)
    projected_low = projected.astype(low_type)
    pair_all = row_rows(projected_low[..., column_width_count:])
    heads_q = projected_low[..., :column_width_count].reshape(seqs, rows_here, heads_here, HEAD)
    heads_k = pair_all[..., :column_width_count].reshape(seqs, total_rows, heads_here, HEAD)
    heads_v = pair_all[..., column_width_count:].reshape(seqs, total_rows, heads_here, HEAD)
    self_scores = (
        jnp.einsum("sqhd,skhd->shqk", heads_q, heads_k, preferred_element_type=full_type)
        * self_scale
    )
    self_top = jnp.max(jnp.where(latent_attend_mask, self_scores, NEGATIVE), axis=-1)
    self_total = jnp.sum(
        jnp.where(latent_attend_mask, jnp.exp(self_scores - self_top[..., None]), 0.0), axis=-1
    )
    self_lse = self_top + jnp.log(self_total)
    self_chances = jnp.where(
        latent_attend_mask, jnp.exp(self_scores - self_lse[..., None]), 0.0
    ).astype(low_type)
    self_mixed = jnp.einsum(
        "shqk,skhd->sqhd", self_chances, heads_v, preferred_element_type=full_type
    )
    self_branch, mixed_rows = project_rows(
        self_mixed.reshape(seqs, rows_here, column_width_count).astype(low_type),
        self_out,
        FORWARD_SECOND,
    )
    after_self = after_first + self_branch
    final_state, second_saved = feed_forward(after_self, second_gain, second_expand, second_shrink)
    result = final_state.astype(low_type)
    grad_state = cotangent.astype(full_type)
    grad_state, grad_second_gain, grad_second_expand, grad_second_shrink = feed_backward(
        grad_state, second_saved, second_gain, second_expand, second_shrink
    )
    grad_mixed, self_branch_rows = project_cols(
        grad_state.astype(low_type), self_out, BACKWARD_SECOND
    )
    grad_self_out = weight_grad(GRADIENT_SECOND, mixed_rows, self_branch_rows)
    grad_mixed_low = grad_mixed.astype(low_type).reshape(seqs, rows_here, heads_here, HEAD)
    self_delta = jnp.transpose(
        jnp.sum(grad_mixed_low.astype(full_type) * self_mixed, axis=-1), (0, 2, 1)
    )
    again_scores = (
        jnp.einsum("sqhd,skhd->shqk", heads_q, heads_k, preferred_element_type=full_type)
        * self_scale
    )
    again_chances = jnp.where(latent_attend_mask, jnp.exp(again_scores - self_lse[..., None]), 0.0)
    grad_self_chances = jnp.einsum(
        "sqhd,skhd->shqk", grad_mixed_low, heads_v, preferred_element_type=full_type
    )
    grad_self_scores = (again_chances * (grad_self_chances - self_delta[..., None])).astype(
        low_type
    )
    grad_heads_q = (
        jnp.einsum("shqk,skhd->sqhd", grad_self_scores, heads_k, preferred_element_type=full_type)
        * self_scale
    )
    grad_heads_k = (
        jnp.einsum("shqk,sqhd->skhd", grad_self_scores, heads_q, preferred_element_type=full_type)
        * self_scale
    )
    grad_heads_v = jnp.einsum(
        "shqk,sqhd->skhd",
        again_chances.astype(low_type),
        grad_mixed_low,
        preferred_element_type=full_type,
    )
    pair_grad = row_reduce(
        jnp.concatenate(
            [
                grad_heads_k.reshape(seqs, total_rows, column_width_count),
                grad_heads_v.reshape(seqs, total_rows, column_width_count),
            ],
            axis=-1,
        )
    )
    joined_grad = jnp.concatenate(
        [grad_heads_q.reshape(seqs, rows_here, column_width_count), pair_grad], axis=-1
    ).astype(low_type)
    grad_self_in, joined_rows = project_rows(joined_grad, joined, BACKWARD_FIRST)
    grad_joined = weight_grad(GRADIENT_FIRST, self_rows, joined_rows)
    grad_self_normed, grad_self_gain = norm_backward(grad_self_in, self_gain, self_normed, self_inv)
    grad_state = grad_state + grad_self_normed
    grad_state, grad_first_gain, grad_first_expand, grad_first_shrink = feed_backward(
        grad_state, first_saved, first_gain, first_expand, first_shrink
    )
    grad_attended, cross_branch_rows = project_cols(
        grad_state.astype(low_type), cross_out, BACKWARD_SECOND
    )
    grad_cross_out = weight_grad(GRADIENT_SECOND, attended_rows, cross_branch_rows)
    grad_attended_all = query_feats(grad_attended.astype(low_type))
    cross_delta = jnp.sum(grad_attended_all.astype(full_type) * attended_all, axis=-1)

    def cross_back_one(carry, item):
        query_one, keys_one, values_one, grad_one, lse_one, delta_one, mask_one, normed_one = item
        scores_one = (
            jnp.einsum("qd,kd->qk", query_one, keys_one, preferred_element_type=full_type)
            * cross_scale
        )
        chances_one = jnp.where(mask_one, jnp.exp(scores_one - lse_one[:, None]), 0.0)
        grad_chances = jnp.einsum(
            "qd,kd->qk", grad_one, values_one, preferred_element_type=full_type
        )
        grad_scores = (chances_one * (grad_chances - delta_one[:, None])).astype(low_type)
        grad_query = (
            jnp.einsum("qk,kd->qd", grad_scores, keys_one, preferred_element_type=full_type)
            * cross_scale
        )
        grad_keys = (
            jnp.einsum("qk,qd->kd", grad_scores, query_one, preferred_element_type=full_type)
            * cross_scale
        )
        grad_values = jnp.einsum(
            "qk,qd->kd", chances_one.astype(low_type), grad_one, preferred_element_type=full_type
        )
        grad_normed = split_einsum("kd,cd->kc", grad_keys, cross_key, True) + split_einsum(
            "kd,cd->kc", grad_values, cross_value, True
        )
        key_sum = carry[0] + split_einsum("kc,kd->cd", grad_keys, normed_one, False)
        value_sum = carry[1] + split_einsum("kc,kd->cd", grad_values, normed_one, False)
        return ((key_sum, value_sum), (grad_query, grad_normed))

    empty = jnp.zeros(cross_key.shape, full_type)
    (grad_key_sum, grad_value_sum), (grad_query_all, grad_input_part) = lax.scan(
        cross_back_one,
        (empty, empty),
        (
            query_all,
            keys_all,
            values_all,
            grad_attended_all,
            cross_lse,
            cross_delta,
            cross_mask,
            input_low,
        ),
    )
    grad_query_here = query_grads(grad_query_all).astype(low_type)
    grad_cross_in, query_rows = project_rows(grad_query_here, cross_query, BACKWARD_FIRST)
    grad_cross_query = weight_grad(GRADIENT_FIRST, cross_rows, query_rows)
    grad_cross_normed, grad_cross_gain = norm_backward(
        grad_cross_in, cross_gain, cross_normed, cross_inv
    )
    grad_latents = grad_state + grad_cross_normed
    input_gain_part = jnp.sum(grad_input_part * input_normed, axis=(0, 1))
    summed = lax.psum(grad_input_part.astype(jnp.bfloat16), "row").astype(jnp.float32)
    grad_inputs = input_back(summed, input_normed, input_inv, input_gain).astype(low_type)
    grid = (
        lax.psum(grad_cross_query.astype(jnp.bfloat16), "dp").astype(jnp.float32),
        lax.psum(grad_cross_out.astype(jnp.bfloat16), "dp").astype(jnp.float32),
        lax.psum(grad_first_expand.astype(jnp.bfloat16), "dp").astype(jnp.float32),
        lax.psum(grad_first_shrink.astype(jnp.bfloat16), "dp").astype(jnp.float32),
        lax.psum(grad_joined.astype(jnp.bfloat16), "dp").astype(jnp.float32),
        lax.psum(grad_self_out.astype(jnp.bfloat16), "dp").astype(jnp.float32),
        lax.psum(grad_second_expand.astype(jnp.bfloat16), "dp").astype(jnp.float32),
        lax.psum(grad_second_shrink.astype(jnp.bfloat16), "dp").astype(jnp.float32),
    )
    gains_local = jnp.stack([grad_cross_gain, grad_first_gain, grad_self_gain, grad_second_gain])
    padded = lax.dynamic_update_slice(
        jnp.zeros((4, width_row * lax.axis_size("row")), full_type),
        gains_local,
        (jnp.int32(0), row_at * width_row),
    )
    shared = lax.psum((grad_key_sum, grad_value_sum, padded, input_gain_part), ("row", "col", "dp"))
    gains_all = lax.dynamic_slice_in_dim(shared[2], row_at * width_row, width_row, 1)
    joined_sum = grid[4]
    return (
        result,
        grad_latents,
        grad_inputs,
        gains_all[0],
        shared[3],
        grid[0],
        shared[0],
        shared[1],
        grid[1],
        gains_all[1],
        grid[2],
        grid[3],
        gains_all[2],
        joined_sum[:, :column_width_count],
        joined_sum[:, column_width_count : 2 * column_width_count],
        joined_sum[:, 2 * column_width_count :],
        grid[5],
        gains_all[3],
        grid[6],
        grid[7],
    )


NEG = -1e30
WIDE = 256
BLOCK = 128


def col_step(flip):
    return tuple((c, c ^ flip) for c in range(4))


ROW_SWAP = ((0, 1), (1, 0))
BOTH_SWAP = tuple((r * 4 + c, (1 - r) * 4 + (c ^ 2)) for r in range(2) for c in range(4))
SEQ_NEAR = ((0, 1), (1, 0), (2, 3), (3, 2))
SEQ_FAR = ((0, 2), (2, 0), (1, 3), (3, 1))
GROUP = ("col", "row")


def swap_row(value):
    return lax.ppermute(value, "row", ROW_SWAP)


def swap_chip(value):
    return lax.ppermute(value, "col", col_step(2))


def swap_core(value):
    return lax.ppermute(value, "col", col_step(1))


def swap_both(value):
    return lax.ppermute(value, ("row", "col"), BOTH_SWAP)


def gather_eight(value):
    near = jnp.stack([value, swap_row(value), swap_chip(value), swap_both(value)])
    return near, swap_core(near)


def exchange(value):
    return lax.all_to_all(value, GROUP, 0, 0, tiled=True)


def kernel(body, outs, *args, scratch=(), scalars=True, cost=None):
    vmem = pl.BlockSpec(memory_space=pltpu.VMEM)
    smem = pl.BlockSpec(memory_space=pltpu.SMEM)
    specs = [smem if scalars and i == 0 else vmem for i in range(len(args))]
    return pl.pallas_call(
        body,
        out_shape=tuple(jax.ShapeDtypeStruct(shape, kind) for shape, kind in outs),
        in_specs=specs,
        out_specs=tuple(vmem for _ in outs),
        scratch_shapes=list(scratch),
        compiler_params=pltpu.CompilerParams(vmem_limit_bytes=56 * 1024 * 1024),
    )(*args)


def mm(a, b):
    return lax.dot_general(a, b, (((1,), (0,)), ((), ())), preferred_element_type=jnp.float32)


def mt(a, b):
    return lax.dot_general(a, b, (((1,), (1,)), ((), ())), preferred_element_type=jnp.float32)


def low(v):
    return v.astype(jnp.bfloat16)


def full(v):
    return v.astype(jnp.float32)


def norm_parts(value):
    width = value.shape[-1]
    center = jnp.sum(value, axis=-1, keepdims=True) / width
    shifted = value - center
    spread = jnp.sum(shifted * shifted, axis=-1, keepdims=True) / width
    inv = lax.rsqrt(spread + EPS)
    return shifted * inv, inv


def norm_back(grad, gain, normed, inv):
    width = grad.shape[-1]
    scaled = grad * gain
    first = jnp.sum(scaled, axis=-1, keepdims=True) / width
    second = jnp.sum(scaled * normed, axis=-1, keepdims=True) / width
    return inv * (scaled - first - normed * second), jnp.sum(grad * normed, axis=0, keepdims=True)


def phi(value):
    return 0.5 * (1.0 + lax.erf(value * (1.0 / math.sqrt(2.0))))


def gelu_value(value):
    return value * phi(value)


def gelu_slope(value):
    return phi(value) + value * jnp.exp(value * value * -0.5) * (1.0 / math.sqrt(2.0 * math.pi))


def three(value):
    first = low(value)
    rest = value - full(first)
    second = low(rest)
    return full(first), full(second), rest - full(second)


def block_of(scalars, step, core):
    return scalars[0] ^ (4 * (step // 2) + 2 * core + step % 2)


def rows_of(count, lanes):
    return lax.broadcasted_iota(jnp.int32, (count, lanes), 0)


def fold_kernel(scalars, key, value, query, out, parts):
    at = pl.multiple_of(scalars[2] * WIDE, WIDE)
    channels = key.shape[0]
    parts[...] = jnp.zeros_like(parts)
    first = low(mt(key[:, pl.ds(at, WIDE)], query[...]))
    second = low(mm(value[:, pl.ds(at, WIDE)], out[...]))
    for b in range(4):
        parts[b, 0, 0:channels, :] = first[:, b * BLOCK : (b + 1) * BLOCK]
        parts[b, 1, 0:channels, :] = second[:, b * BLOCK : (b + 1) * BLOCK]


def add_kernel(parts, total):
    acc = full(parts[0])
    for b in range(1, parts.shape[0]):
        acc = acc + full(parts[b])
    total[...] = low(acc)


def input_kernel(rows, gain, plain, turned, *, channels):
    value = full(rows[...])
    lanes = lax.broadcasted_iota(jnp.int32, value.shape, 1)
    center = jnp.sum(value, axis=-1, keepdims=True) / channels
    shifted = jnp.where(lanes < channels, value - center, 0.0)
    spread = jnp.sum(shifted * shifted, axis=-1, keepdims=True) / channels
    result = shifted * lax.rsqrt(spread + EPS) * gain[...]
    plain[...] = low(result)
    turned[...] = low(result.T)


def first_kernel(latents, gain, normed):
    value, _ = norm_parts(full(latents[...]))
    normed[...] = low(value * gain[...])


def query_kernel(scalars, near, far, normed, folded_query, folded_out, query):
    row, col = scalars[1], scalars[2]
    for step in range(4):
        for core, source in ((0, near), (1, far)):
            block = 4 * (row ^ (step % 2)) + (col ^ (2 * (step // 2) + core))
            at = pl.multiple_of(block * BLOCK, BLOCK)
            folded_query[:, pl.ds(at, BLOCK)] = source[step, 0]
            folded_out[:, pl.ds(at, BLOCK)] = source[step, 1]
    query[...] = low(mt(folded_query[...], normed[...]) * (1.0 / math.sqrt(D)))


def cross_kernel(scalars, near, far, limits, plain, turned, queries, result, *, channels):
    for step in range(4):
        for core, source in ((0, near), (1, far)):
            queries[block_of(scalars, step, core)] = source[step]
    base = scalars[3]
    count, padded = plain.shape

    def pair(i, carry):
        query = jnp.concatenate([queries[2 * i], queries[2 * i + 1]], axis=1)
        limit = jnp.concatenate([limits[2 * i], limits[2 * i + 1]], axis=1)
        scores = mm(plain[...], query)
        keys = rows_of(count, 2 * BLOCK) + base
        mask = keys < limit
        top = jnp.max(jnp.where(mask, scores, NEG), axis=0, keepdims=True)
        weights = jnp.where(mask, jnp.exp(scores - top), 0.0)
        total = jnp.sum(weights, axis=0, keepdims=True)
        mixed = mm(turned[...], low(weights))
        some = total > 0.0
        mixed = mixed * jnp.where(some, 1.0 / jnp.where(some, total, 1.0), 0.0)
        lse = jnp.where(some, top + jnp.log(jnp.where(some, total, 1.0)), NEG)
        index = rows_of(padded, 2 * BLOCK)
        for k, part in enumerate(three(lse)):
            mixed = jnp.where(index == channels + k, part, mixed)
        mixed = low(mixed)
        result[2 * i] = mixed[:, :BLOCK]
        result[2 * i + 1] = mixed[:, BLOCK:]
        return carry

    lax.fori_loop(0, 4, pair, 0)


def expand_tiles(value, packed, at):
    outs = []
    for c in range(4):
        acc = None
        for r in range(2):
            part = mm(value[:, r * 512 : (r + 1) * 512], packed[2 * c + r, at : at + 512, :])
            acc = part if acc is None else acc + part
        outs.append(acc)
    return jnp.concatenate(outs, axis=1)


def shrink_tiles(value, packed, at):
    outs = []
    for r in range(2):
        for j in range(2):
            acc = None
            for c in range(4):
                tile = packed[2 * c + r, at + j * WIDE : at + (j + 1) * WIDE, :]
                part = mm(value[:, c * WIDE : (c + 1) * WIDE], tile)
                acc = part if acc is None else acc + part
            outs.append(acc)
    return jnp.concatenate(outs, axis=1)


def expand_back(value, packed, at):
    outs = []
    for r in range(2):
        acc = None
        for c in range(4):
            part = mt(value[:, c * WIDE : (c + 1) * WIDE], packed[2 * c + r, at : at + 512, :])
            acc = part if acc is None else acc + part
        outs.append(acc)
    return jnp.concatenate(outs, axis=1)


def shrink_back(value, packed, at):
    outs = []
    for c in range(4):
        acc = None
        for r in range(2):
            for j in range(2):
                tile = packed[2 * c + r, at + j * WIDE : at + (j + 1) * WIDE, :]
                start = r * 512 + j * WIDE
                part = mt(value[:, start : start + WIDE], tile)
                acc = part if acc is None else acc + part
        outs.append(acc)
    return jnp.concatenate(outs, axis=1)


def merge_kernel(
    parts, latents, folded_out, packed, gains,
    mixed_out, lse_out, after_cross, hidden, upward, active, after_first, self_in, *, channels
):
    lses = []
    for d in range(8):
        rows = full(parts[d, channels : channels + 3, :])
        lses.append(rows[0:1] + rows[1:2] + rows[2:3])
    top = lses[0]
    for item in lses[1:]:
        top = jnp.maximum(top, item)
    total = jnp.zeros_like(top)
    mixed = jnp.zeros(parts.shape[1:], jnp.float32)
    for d in range(8):
        share = jnp.exp(lses[d] - top)
        total = total + share
        mixed = mixed + full(parts[d]) * share
    mixed = low(mixed / total)
    mixed_out[...] = mixed
    lse_out[...] = top + jnp.log(total)
    branch = mm(low(full(mixed).T), folded_out[...])
    state = full(latents[...]) + branch
    after_cross[...] = state
    normed, _ = norm_parts(state)
    hid = low(normed * gains[1:2, :])
    hidden[...] = hid
    up = expand_tiles(hid, packed, 0)
    upward[...] = up
    act = low(gelu_value(up))
    active[...] = act
    state = state + shrink_tiles(act, packed, 512)
    after_first[...] = state
    normed, _ = norm_parts(state)
    self_in[...] = low(normed * gains[2:3, :])


def attend_kernel(
    scalars, near, far, weights, limits, places, rows_out, qkv_out, mixed_out, lse_out, sent
):
    for core, source in ((0, near), (1, far)):
        for step in range(4):
            at = pl.multiple_of(block_of(scalars, step, core) * BLOCK, BLOCK)
            rows = source[step]
            rows_out[pl.ds(at, BLOCK), :] = rows
    qkv_out[...] = low(mm(rows_out[...], weights[...]))
    scale = 1.0 / math.sqrt(HEAD)
    turned = low(full(qkv_out[:, 2 * HEAD :]).T)

    def pair(i, carry):
        at = pl.multiple_of(i * WIDE, WIDE)
        query = qkv_out[pl.ds(at, WIDE), 0:HEAD]
        scores = mt(qkv_out[:, HEAD : 2 * HEAD], query) * scale
        limit = jnp.concatenate([limits[2 * i], limits[2 * i + 1]], axis=1)
        mask = places[...] < limit
        top = jnp.max(jnp.where(mask, scores, NEG), axis=0, keepdims=True)
        share = jnp.where(mask, jnp.exp(scores - top), 0.0)
        total = jnp.sum(share, axis=0, keepdims=True)
        mixed = mm(turned, low(share)) / total
        mixed_out[:, pl.ds(at, WIDE)] = mixed
        lse_out[:, pl.ds(at, WIDE)] = top + jnp.log(total)
        lower = low(mixed)
        sent[2 * i] = lower[:, :BLOCK]
        sent[2 * i + 1] = lower[:, BLOCK:]
        return carry

    lax.fori_loop(0, 4, pair, 0)


def second_kernel(
    parts, after_first, cotangent, gain, packed,
    out, joined, hidden, active, grad_up, grad_gain, branch_grad, state_grad, sent
):
    att = jnp.concatenate([full(parts[h]).T for h in range(8)], axis=1)
    att = low(att)
    joined[...] = att
    state = after_first[...] + shrink_tiles(att, packed, 0)
    normed, inv = norm_parts(state)
    hid = low(normed * gain[...])
    hidden[...] = hid
    up = expand_tiles(hid, packed, 512)
    act = low(gelu_value(up))
    active[...] = act
    final = state + shrink_tiles(act, packed, 1024)
    out[...] = low(final)
    grad = cotangent[...]
    grad_act = shrink_back(grad, packed, 1024)
    gu = low(grad_act * gelu_slope(up))
    grad_up[...] = gu
    grad_hid = expand_back(gu, packed, 512)
    back, grad_gain[...] = norm_back(grad_hid, gain[...], normed, inv)
    total = full(grad) + back
    state_grad[...] = total
    lower = low(total)
    branch_grad[...] = lower
    grad_att = shrink_back(lower, packed, 0)
    for h in range(8):
        sent[h] = low(grad_att[:, h * BLOCK : (h + 1) * BLOCK].T)


def attend_back_kernel(
    scalars, parts, qkv, mixed, lse, weights, limits, places, grads, sent
):
    scale = 1.0 / math.sqrt(HEAD)
    keys_turned = low(full(qkv[:, HEAD : 2 * HEAD]).T)

    def pair(i, carry):
        grad_k, grad_v = carry
        at = pl.multiple_of(i * WIDE, WIDE)
        query = qkv[pl.ds(at, WIDE), 0:HEAD]
        grad_out = jnp.concatenate([parts[2 * i], parts[2 * i + 1]], axis=1)
        delta = jnp.sum(full(grad_out) * mixed[:, pl.ds(at, WIDE)], axis=0, keepdims=True)
        scores = mt(qkv[:, HEAD : 2 * HEAD], query) * scale
        limit = jnp.concatenate([limits[2 * i], limits[2 * i + 1]], axis=1)
        mask = places[...] < limit
        share = jnp.where(mask, jnp.exp(scores - lse[:, pl.ds(at, WIDE)]), 0.0)
        grad_share = mm(qkv[:, 2 * HEAD :], grad_out)
        grad_scores = low(share * (grad_share - delta))
        grad_k = grad_k + mm(grad_scores, query)
        grad_v = grad_v + mt(low(share), grad_out)
        grad_q = mm(keys_turned, grad_scores) * scale
        grads[pl.ds(at, WIDE), 0:HEAD] = low(grad_q.T)
        return grad_k, grad_v

    zero = jnp.zeros((qkv.shape[0], HEAD), jnp.float32)
    grad_k, grad_v = lax.fori_loop(0, 4, pair, (zero, zero))
    grads[:, HEAD : 2 * HEAD] = low(grad_k * scale)
    grads[:, 2 * HEAD :] = low(grad_v)
    for step in range(4):
        for core in range(2):
            at = pl.multiple_of(block_of(scalars, step, core) * BLOCK, BLOCK)
            sent[core, step] = low(mt(grads[pl.ds(at, BLOCK), :], weights[...]))


def first_back_kernel(
    own, by_row, by_chip, by_both, state_grad, after_first, after_cross, upward, packed, gains,
    folded_out, mixed, lse,
    gain_grads, first_branch, grad_up, cross_branch, cross_grad, value_part, sent, *, channels
):
    grad_in = full(own[...]) + full(by_row[...]) + full(by_chip[...]) + full(by_both[...])
    normed, inv = norm_parts(after_first[...])
    back, self_gain = norm_back(grad_in, gains[2:3, :], normed, inv)
    grad = state_grad[...] + back
    lower = low(grad)
    first_branch[...] = lower
    gu = low(shrink_back(lower, packed, 512) * gelu_slope(upward[...]))
    grad_up[...] = gu
    grad_hid = expand_back(gu, packed, 0)
    normed, inv = norm_parts(after_cross[...])
    back, first_gain = norm_back(grad_hid, gains[1:2, :], normed, inv)
    gain_grads[0:1, :] = first_gain
    gain_grads[1:2, :] = self_gain
    grad = grad + back
    cross_grad[...] = grad
    lower = low(grad)
    cross_branch[...] = lower
    value_part[...] = low(mm(mixed[...], lower))
    grad_mixed = mt(folded_out[...], lower)
    padded = grad_mixed.shape[0]
    index = rows_of(padded, BLOCK)
    grad_mixed = jnp.where(index < channels, grad_mixed, 0.0)
    rounded = full(low(grad_mixed))
    delta = jnp.sum(rounded * full(mixed[...]), axis=0, keepdims=True)
    for k, part in enumerate(three(lse[...]) + three(delta)):
        grad_mixed = jnp.where(index == channels + k, part, grad_mixed)
    sent[...] = low(grad_mixed)


def cross_back_kernel(
    scalars, near, far, queries, limits, plain, turned, rows, gain,
    grad_rows, grad_gain, sent, grads, total, *, channels
):
    for step in range(4):
        for core, source in ((0, near), (1, far)):
            grads[block_of(scalars, step, core)] = source[step]
    base = scalars[3]
    count, padded = plain.shape
    total[...] = jnp.zeros_like(total)

    def pair(i, carry):
        query = jnp.concatenate([queries[2 * i], queries[2 * i + 1]], axis=1)
        grad_mixed = jnp.concatenate([grads[2 * i], grads[2 * i + 1]], axis=1)
        extra = full(grad_mixed[channels : channels + 6, :])
        lse = extra[0:1] + extra[1:2] + extra[2:3]
        delta = extra[3:4] + extra[4:5] + extra[5:6]
        limit = jnp.concatenate([limits[2 * i], limits[2 * i + 1]], axis=1)
        mask = rows_of(count, 2 * BLOCK) + base < limit
        scores = mm(plain[...], query)
        share = jnp.where(mask, jnp.exp(scores - lse), 0.0)
        grad_share = mm(plain[...], grad_mixed)
        grad_scores = low(share * (grad_share - delta))
        out = low(mm(turned[...], grad_scores) * (1.0 / math.sqrt(D)))
        sent[2 * i] = out[:, :BLOCK]
        sent[2 * i + 1] = out[:, BLOCK:]
        total[...] += mt(grad_scores, query) + mt(low(share), grad_mixed)
        return carry

    lax.fori_loop(0, 4, pair, 0)
    value = full(rows[...])
    lanes = lax.broadcasted_iota(jnp.int32, value.shape, 1)
    inside = lanes < channels
    center = jnp.sum(value, axis=-1, keepdims=True) / channels
    shifted = jnp.where(inside, value - center, 0.0)
    inv = lax.rsqrt(jnp.sum(shifted * shifted, axis=-1, keepdims=True) / channels + EPS)
    normed = shifted * inv
    grad = jnp.where(inside, total[...], 0.0)
    grad_gain[...] = jnp.sum(grad * normed, axis=0, keepdims=True)
    scaled = grad * gain[...]
    first = jnp.sum(scaled, axis=-1, keepdims=True) / channels
    second = jnp.sum(scaled * normed, axis=-1, keepdims=True) / channels
    result = inv * (scaled - first - normed * second)
    grad_rows[...] = low(result[:, :channels])


def last_kernel(
    parts, folded_query, normed_in, latents, gains, cross_grad, value_part, gain_rows,
    grad_latents, sent, *, channels
):
    acc = full(parts[0])
    for d in range(1, 8):
        acc = acc + full(parts[d])
    padded = acc.shape[0]
    index = rows_of(padded, BLOCK)
    acc = jnp.where(index < channels, acc, 0.0)
    grad_query = low(acc)
    grad_in = mm(low(acc.T), folded_query[...])
    normed, inv = norm_parts(full(latents[...]))
    back, cross_gain = norm_back(grad_in, gains[0:1, :], normed, inv)
    grad_latents[...] = cross_grad[...] + back
    part = mm(grad_query, normed_in[...])
    wide = rows_of(padded, part.shape[1])
    rows = [cross_gain] + [gain_rows[k : k + 1, :] for k in range(4)]
    for k, row in enumerate(rows):
        high = low(row)
        part = jnp.where(wide == channels + 2 * k, full(high), part)
        part = jnp.where(wide == channels + 2 * k + 1, row - full(high), part)
    part = low(part)
    for b in range(8):
        sent[b, 0] = part[:, b * BLOCK : (b + 1) * BLOCK]
        sent[b, 1] = value_part[:, b * BLOCK : (b + 1) * BLOCK]


def finish_kernel(
    scalars, near, far, key, value, packed,
    grad_query, grad_key, grad_out, grad_value, gain_grads, key_sum, value_sum, *, channels
):
    for step in range(4):
        for core, source in ((0, near), (1, far)):
            at = pl.multiple_of(block_of(scalars, step, core) * BLOCK, BLOCK)
            key_sum[:, pl.ds(at, BLOCK)] = source[step, 0]
            value_sum[:, pl.ds(at, BLOCK)] = source[step, 1]
    extra = full(key_sum[channels : channels + 10, :])
    for k in range(5):
        gain_grads[k : k + 1, :] = extra[2 * k : 2 * k + 1] + extra[2 * k + 1 : 2 * k + 2]
    at = pl.multiple_of(scalars[2] * WIDE, WIDE)
    half = pl.multiple_of(scalars[1] * 512, 512)
    turned = full(key_sum[:, pl.ds(half, 512)]).T
    grad_query[...] = mm(low(turned[:, :channels]), key[:, pl.ds(at, WIDE)])
    turned = full(value[:, pl.ds(at, WIDE)]).T
    grad_out[...] = mm(low(turned), value_sum[0:channels, pl.ds(half, 512)])
    grad_key[...] = expand_tiles(key_sum[...], packed, 0)[:channels]
    grad_value[...] = shrink_back(value_sum[...], packed, 512)[:channels]


def wide_rows(value, row):
    half = value.shape[1] // 2
    keep = lax.dynamic_slice_in_dim(value, row * half, half, 1)
    give = lax.dynamic_slice_in_dim(value, (1 - row) * half, half, 1)
    return keep, give


def for_rows(value, row):
    keep, give = wide_rows(value, row)
    pair = jnp.stack([keep, swap_row(give)])
    both = jnp.stack([pair, swap_chip(pair)])
    return jnp.stack([both, swap_core(both)])


def for_cols(value, chip, core):
    keep, give = wide_rows(value, chip)
    pair = jnp.stack([keep, swap_chip(give)])
    half = pair.shape[2] // 2
    mine = lax.dynamic_slice_in_dim(pair, core * half, half, 2)
    theirs = lax.dynamic_slice_in_dim(pair, (1 - core) * half, half, 2)
    both = jnp.stack([mine, swap_core(theirs)])
    every = jnp.stack([both, swap_row(both)])
    return jnp.transpose(every, (1, 2, 0, 3, 4))


def over_rows(first, second):
    return lax.dot_general(
        first.reshape(-1, first.shape[-1]),
        second.reshape(-1, second.shape[-1]),
        (((0,), (0,)), ((), ())),
        preferred_element_type=jnp.float32,
    )


def in_order(row, own, other, axis):
    return jnp.where(
        row == 0,
        jnp.concatenate([own, other], axis),
        jnp.concatenate([other, own], axis),
    )


def tiles_of(weight):
    return [weight[:, :WIDE], weight[:, WIDE:]]


def all_of(parts):
    packed = jnp.concatenate(parts, axis=0)
    return lax.all_gather(packed, GROUP, axis=0, tiled=False)


def fast_device(
    latents, inputs, positions, piece_start, cotangent, cross_gain, input_gain, cross_query,
    cross_key, cross_value, cross_out, first_gain, first_expand, first_shrink, self_gain,
    self_query, self_key, self_value, self_out, second_gain, second_expand, second_shrink,
):
    bf, f32 = jnp.bfloat16, jnp.float32
    row, col = lax.axis_index("row"), lax.axis_index("col")
    chip, core = col // 2, col % 2
    channels = inputs.shape[-1]
    padded = -(-(channels + 11) // 16) * 16
    keys_here = inputs.shape[1] // 2
    base = col * inputs.shape[1] + row * keys_here
    scalars = jnp.stack([2 * col + row, row, col, base]).astype(jnp.int32)
    rows = BLOCK

    def swap_half(block):
        keep = lax.dynamic_slice_in_dim(block, row * rows, rows, 0)
        give = lax.dynamic_slice_in_dim(block, (1 - row) * rows, rows, 0)
        return in_order(row, keep, swap_row(give), 1)

    def swap_back(value):
        keep, give = wide_rows(value, row)
        return in_order(row, keep, swap_row(give), 0)

    parts = kernel(
        fold_kernel, [((4, 2, padded, BLOCK), bf)], scalars, cross_key, cross_value, cross_query,
        cross_out,
    )[0]
    parts = lax.all_to_all(parts, "col", 0, 0, tiled=True)
    folded = kernel(add_kernel, [((2, padded, BLOCK), bf)], parts, scalars=False)[0]
    fold_near, fold_far = gather_eight(folded)

    gains_here = jnp.stack([cross_gain, first_gain, self_gain, second_gain])
    gains = in_order(row, gains_here, swap_row(gains_here), 1)
    state = swap_half(latents[0])
    normed_in = kernel(
        first_kernel, [((rows, D), bf)], state, gains[0:1], scalars=False
    )[0]
    own_rows = jnp.pad(
        lax.dynamic_slice_in_dim(inputs[0], row * keys_here, keys_here, 0),
        ((0, 0), (0, padded - channels)),
    )
    wide_gain = jnp.pad(input_gain, (0, padded - channels))[None]
    plain, turned = kernel(
        functools.partial(input_kernel, channels=channels),
        [((keys_here, padded), bf), ((padded, keys_here), bf)],
        own_rows, wide_gain, scalars=False,
    )
    limits = view_limits(positions, piece_start)[0].reshape(8, 1, BLOCK)
    places = positions[0][:, None]

    packed_first = all_of([first_expand] + tiles_of(first_shrink))
    packed_second = all_of(tiles_of(self_out) + [second_expand] + tiles_of(second_shrink))
    packed_cross = all_of([cross_query] + tiles_of(cross_out))
    joined_weights = [
        w.reshape(w.shape[0], 2, HEAD) for w in (self_query, self_key, self_value)
    ]
    mine = jnp.concatenate(
        [lax.dynamic_index_in_dim(w, row, 1, False) for w in joined_weights], axis=1
    )
    theirs = jnp.concatenate(
        [lax.dynamic_index_in_dim(w, 1 - row, 1, False) for w in joined_weights], axis=1
    )
    head_weights = in_order(row, mine, swap_row(theirs), 0)

    folded_query, folded_out, query = kernel(
        query_kernel, [((padded, D), bf), ((padded, D), bf), ((padded, rows), bf)],
        scalars, fold_near, fold_far, normed_in,
    )
    query_near, query_far = gather_eight(query)
    queries, partial_mixed = kernel(
        functools.partial(cross_kernel, channels=channels),
        [((8, padded, BLOCK), bf), ((8, padded, BLOCK), bf)],
        scalars, query_near, query_far, limits, plain, turned,
    )
    received = exchange(partial_mixed)
    mixed, lse, after_cross, hidden, upward, active, after_first, self_in = kernel(
        functools.partial(merge_kernel, channels=channels),
        [
            ((padded, rows), bf), ((1, rows), f32), ((rows, D), f32), ((rows, D), bf),
            ((rows, D), f32), ((rows, D), bf), ((rows, D), f32), ((rows, D), bf),
        ],
        received, state, folded_out, packed_first, gains, scalars=False,
    )
    self_near, self_far = gather_eight(self_in)
    total_rows = positions.shape[1]
    self_rows, qkv, self_mixed, self_lse, sent = kernel(
        attend_kernel,
        [
            ((total_rows, D), bf), ((total_rows, 3 * HEAD), bf), ((HEAD, total_rows), f32),
            ((1, total_rows), f32), ((8, HEAD, BLOCK), bf),
        ],
        scalars, self_near, self_far, head_weights, limits, places,
    )
    received = exchange(sent)
    grad_final = swap_half(cotangent[0])
    (
        out, joined, second_hidden, second_active, second_up, second_gain_part, self_branch,
        state_grad, sent,
    ) = kernel(
        second_kernel,
        [
            ((rows, D), bf), ((rows, D), bf), ((rows, D), bf), ((rows, D), bf), ((rows, D), bf),
            ((1, D), f32), ((rows, D), bf), ((rows, D), f32), ((8, BLOCK, rows), bf),
        ],
        received, after_first, grad_final, gains[3:4], packed_second, scalars=False,
    )
    received = exchange(sent)
    grad_qkv, sent = kernel(
        attend_back_kernel,
        [((total_rows, 3 * HEAD), bf), ((2, 4, rows, D), bf)],
        scalars, received, qkv, self_mixed, self_lse, head_weights, limits, places,
    )
    summed = low(full(sent[0]) + full(swap_core(sent[1])))
    by_row, by_chip, by_both = swap_row(summed[1]), swap_chip(summed[2]), swap_both(summed[3])
    (
        gain_rows, first_branch, first_up, cross_branch, cross_grad, value_part, sent,
    ) = kernel(
        functools.partial(first_back_kernel, channels=channels),
        [
            ((2, D), f32), ((rows, D), bf), ((rows, D), bf), ((rows, D), bf), ((rows, D), f32),
            ((padded, D), bf), ((padded, rows), bf),
        ],
        summed[0], by_row, by_chip, by_both, state_grad, after_first, after_cross, upward,
        packed_first, gains, folded_out, mixed, lse, scalars=False,
    )
    grad_near, grad_far = gather_eight(sent)
    grad_rows, input_gain_part, sent = kernel(
        functools.partial(cross_back_kernel, channels=channels),
        [((keys_here, channels), bf), ((1, padded), f32), ((8, padded, BLOCK), bf)],
        scalars, grad_near, grad_far, queries, limits, plain, turned, own_rows, wide_gain,
        scratch=[pltpu.VMEM((8, padded, BLOCK), bf), pltpu.VMEM((keys_here, padded), f32)],
    )
    received = exchange(sent)
    wide_part = jnp.pad(input_gain_part, ((0, 0), (0, D - padded)))
    extra = jnp.concatenate([gain_rows, second_gain_part, wide_part], axis=0)
    latents_grad, sent = kernel(
        functools.partial(last_kernel, channels=channels),
        [((rows, D), f32), ((8, 2, padded, BLOCK), bf)],
        received, folded_query, normed_in, state, gains, cross_grad, value_part, extra,
        scalars=False,
    )
    received = exchange(sent)
    total = kernel(add_kernel, [((2, padded, BLOCK), bf)], received, scalars=False)[0]
    total = low(full(total) + full(lax.ppermute(total, "dp", SEQ_NEAR)))
    total = low(full(total) + full(lax.ppermute(total, "dp", SEQ_FAR)))
    sum_near, sum_far = gather_eight(total)
    grad_cross_query, grad_cross_key, grad_cross_out, grad_cross_value, gain_grads = kernel(
        functools.partial(finish_kernel, channels=channels),
        [
            (cross_query.shape, f32), (cross_key.shape, f32), (cross_out.shape, f32),
            (cross_value.shape, f32), ((5, D), f32),
        ],
        scalars, sum_near, sum_far, cross_key, cross_value, packed_cross,
        scratch=[pltpu.VMEM((padded, D), bf), pltpu.VMEM((padded, D), bf)],
    )
    half = D // 2
    gains_mine = lax.dynamic_slice_in_dim(gain_grads, row * half, half, 1)

    grad_second_expand = over_rows(
        for_rows(second_hidden, row), for_cols(second_up, chip, core)
    )
    grad_second_shrink = over_rows(
        for_cols(second_active, chip, core), for_rows(grad_final, row)
    )
    grad_self_out = over_rows(for_cols(joined, chip, core), for_rows(self_branch, row))
    grad_first_expand = over_rows(for_rows(hidden, row), for_cols(first_up, chip, core))
    grad_first_shrink = over_rows(for_cols(active, chip, core), for_rows(first_branch, row))
    grad_heads = low(over_rows(self_rows, grad_qkv))
    keep = lax.dynamic_slice_in_dim(grad_heads, row * half, half, 0)
    give = lax.dynamic_slice_in_dim(grad_heads, (1 - row) * half, half, 0)
    pair = swap_row(give)
    summed = lax.psum(
        (
            low(grad_second_expand), low(grad_second_shrink), low(grad_self_out),
            keep, pair, low(grad_first_expand), low(grad_first_shrink),
        ),
        "dp",
    )
    keep, pair = full(summed[3]), full(summed[4])
    grad_qkv_weights = [
        in_order(row, keep[:, k * HEAD : (k + 1) * HEAD], pair[:, k * HEAD : (k + 1) * HEAD], 1)
        for k in range(3)
    ]
    other_rows = swap_row(grad_rows)
    return (
        swap_back(out)[None],
        swap_back(latents_grad)[None],
        in_order(row, grad_rows, other_rows, 0)[None],
        gains_mine[0],
        gain_grads[4, :channels],
        grad_cross_query,
        grad_cross_key,
        grad_cross_value,
        grad_cross_out,
        gains_mine[1],
        full(summed[5]),
        full(summed[6]),
        gains_mine[2],
        grad_qkv_weights[0],
        grad_qkv_weights[1],
        grad_qkv_weights[2],
        full(summed[2]),
        gains_mine[3],
        full(summed[0]),
        full(summed[1]),
    )


def solution(mesh):
    placed = (
        P("dp", "col", "row"),
        P("dp", "col", None),
        P("dp", None),
        P("dp", None),
        P("dp", "col", "row"),
        P("row"),
        P(),
        P("row", "col"),
        P(),
        P(),
        P("col", "row"),
        P("row"),
        P("row", "col"),
        P("col", "row"),
        P("row"),
        P("row", "col"),
        P("row", "col"),
        P("row", "col"),
        P("col", "row"),
        P("row"),
        P("row", "col"),
        P("col", "row"),
    )
    sizes = dict(mesh.shape)
    quick = sizes == {"row": 2, "col": 4, "dp": 4}
    return jax.shard_map(
        fast_device if quick else on_device,
        mesh=mesh,
        in_specs=placed,
        out_specs=(
            P("dp", "col", "row"),
            P("dp", "col", "row"),
            P("dp", "col", None),
            P("row"),
            P(),
            P("row", "col"),
            P(),
            P(),
            P("col", "row"),
            P("row"),
            P("row", "col"),
            P("col", "row"),
            P("row"),
            P("row", "col"),
            P("row", "col"),
            P("row", "col"),
            P("col", "row"),
            P("row"),
            P("row", "col"),
            P("col", "row"),
        ),
        check_vma=False,
    )
```

```python
import functools
import math

import jax
import jax.numpy as jnp
from jax import lax
from jax.experimental import pallas as pl
from jax.experimental.pallas import tpu as pltpu
from jax.sharding import PartitionSpec as P

D = 1024
HEAD = 128
PIECE_LEN = 256


EPS = 1e-05
NEGATIVE = -1e30
FORWARD_FIRST = "xok,kt->xot"
BACKWARD_FIRST = "tpv,qv->tpq"
FORWARD_SECOND = "ybj,jv->ybv"
BACKWARD_SECOND = "xng,wg->xnw"
GRADIENT_FIRST = "zyq,zyi->qi"
GRADIENT_SECOND = "oqv,oqa->va"


def joined_2(shard, axis, combine):
    everything = jax.tree.map(lambda part: lax.all_gather(part, axis), shard)
    first = jax.tree.map(lambda part: part[0], everything)

    def step(k, so_far):
        return combine(so_far, jax.tree.map(lambda part: part[k], everything))

    return lax.fori_loop(1, lax.axis_size(axis), step, first)


def col_rows(value):
    return lax.all_gather(value, "col", axis=1, tiled=True)


def row_reduce(value):
    return lax.psum_scatter(
        value.astype(jnp.bfloat16), "row", scatter_dimension=1, tiled=True
    ).astype(jnp.float32)


def row_rows(value):
    return lax.all_gather(value, "row", axis=1, tiled=True)


def col_reduce(value):
    return lax.psum_scatter(
        value.astype(jnp.bfloat16), "col", scatter_dimension=1, tiled=True
    ).astype(jnp.float32)


def query_feats(value):
    return lax.all_gather(value, "col", axis=2, tiled=True)


def query_grads(value):
    return lax.psum_scatter(
        value.astype(jnp.bfloat16), "col", scatter_dimension=2, tiled=True
    ).astype(jnp.float32)


def row_totals(first, second):
    return lax.psum((first, second), "row")


def project_cols(value, weight, form):
    gathered = col_rows(value)
    partial_sum = jnp.einsum(form, gathered, weight, preferred_element_type=jnp.float32)
    return (row_reduce(partial_sum), gathered)


def project_rows(value, weight, form):
    gathered = row_rows(value)
    partial_sum = jnp.einsum(form, gathered, weight, preferred_element_type=jnp.float32)
    return (col_reduce(partial_sum), gathered)


def weight_grad(form, first, second):
    return jnp.einsum(form, first, second, preferred_element_type=jnp.float32)


def split_parts(value):
    leading = value.astype(jnp.bfloat16)
    residue = (value - leading.astype(jnp.float32)).astype(jnp.bfloat16)
    return (leading, residue)


def split_einsum(form, exact, other, first_side):
    leading, residue = split_parts(exact)
    if first_side:
        return jnp.einsum(form, leading, other, preferred_element_type=jnp.float32) + jnp.einsum(
            form, residue, other, preferred_element_type=jnp.float32
        )
    return jnp.einsum(form, other, leading, preferred_element_type=jnp.float32) + jnp.einsum(
        form, other, residue, preferred_element_type=jnp.float32
    )


def norm_forward(value, gain):
    width = value.shape[-1] * lax.axis_size("row")
    total, squares = row_totals(jnp.sum(value, axis=-1), jnp.sum(value * value, axis=-1))
    center = total / width
    spread = squares / width - center * center
    scale_inv = lax.rsqrt(spread + EPS)
    normed = (value - center[..., None]) * scale_inv[..., None]
    return (normed * gain, normed, scale_inv)


def norm_backward(grad, gain, normed, scale_inv):
    width = grad.shape[-1] * lax.axis_size("row")
    scaled = grad * gain
    first, second = row_totals(jnp.sum(scaled, axis=-1), jnp.sum(scaled * normed, axis=-1))
    result = scale_inv[..., None] * (
        scaled - first[..., None] / width - normed * (second[..., None] / width)
    )
    return (result, jnp.sum(grad * normed, axis=(0, 1)))


def gelu_exact(value):
    return jax.nn.gelu(value, approximate=False)


def gelu_back(value, grad):
    return jax.vjp(gelu_exact, value)[1](grad)[0]


def view_limits(positions, starts):
    ends = starts + PIECE_LEN
    inside = (starts[:, None, :] <= positions[:, :, None]) & (
        positions[:, :, None] < ends[:, None, :]
    )
    reach = jnp.sum(jnp.where(inside, ends[:, None, :], 0), axis=-1)
    return jnp.maximum(positions + 1, reach)


def merge_softmax(first, second):
    top = jnp.maximum(first[0], second[0])
    return (top, first[1] * jnp.exp(first[0] - top) + second[1] * jnp.exp(second[0] - top))


def feed_forward(state, gain, expand, shrink):
    normed_out, normed, scale_inv = norm_forward(state, gain)
    upward, hidden_rows = project_cols(normed_out.astype(jnp.bfloat16), expand, FORWARD_FIRST)
    activated = gelu_exact(upward).astype(jnp.bfloat16)
    branch, active_rows = project_rows(activated, shrink, FORWARD_SECOND)
    return (state + branch, (normed, scale_inv, hidden_rows, upward, active_rows))


def feed_backward(grad, saved, gain, expand, shrink):
    normed, scale_inv, hidden_rows, upward, active_rows = saved
    grad_active, branch_rows = project_cols(grad.astype(jnp.bfloat16), shrink, BACKWARD_SECOND)
    grad_shrink = weight_grad(GRADIENT_SECOND, active_rows, branch_rows)
    grad_upward = gelu_back(upward, grad_active).astype(jnp.bfloat16)
    grad_hidden, upward_rows = project_rows(grad_upward, expand, BACKWARD_FIRST)
    grad_expand = weight_grad(GRADIENT_FIRST, hidden_rows, upward_rows)
    grad_normed, grad_gain = norm_backward(grad_hidden, gain, normed, scale_inv)
    return (grad + grad_normed, grad_gain, grad_expand, grad_shrink)


def input_back(grad_part, normed, scale_inv, gain):
    scaled = grad_part * gain
    first = jnp.mean(scaled, axis=-1, keepdims=True)
    second = jnp.mean(scaled * normed, axis=-1, keepdims=True)
    return scale_inv[..., None] * (scaled - first - normed * second)


def on_device(
    latents,
    inputs,
    positions,
    piece_start,
    cotangent,
    cross_gain,
    input_gain,
    cross_query,
    cross_key,
    cross_value,
    cross_out,
    first_gain,
    first_expand,
    first_shrink,
    self_gain,
    self_query,
    self_key,
    self_value,
    self_out,
    second_gain,
    second_expand,
    second_shrink,
):
    low_type = jnp.bfloat16
    full_type = jnp.float32
    row_at = lax.axis_index("row")
    col_at = lax.axis_index("col")
    seqs = latents.shape[0]
    total_rows = positions.shape[1]
    rows_here = total_rows // lax.axis_size("row")
    column_width_count = cross_query.shape[1]
    width_row = cross_query.shape[0]
    key_rows = inputs.shape[1]
    heads_here = column_width_count // HEAD
    cross_scale = 1.0 / math.sqrt(D)
    self_scale = 1.0 / math.sqrt(HEAD)
    limit_all = view_limits(positions, piece_start)
    limit_here = lax.dynamic_slice_in_dim(limit_all, row_at * rows_here, rows_here, 1)
    key_index = col_at * key_rows + jnp.arange(key_rows, dtype=jnp.int32)
    cross_mask = key_index[None, None, :] < limit_here[:, :, None]
    latent_attend_mask = (positions[:, None, :] < limit_here[:, :, None])[:, None]
    initial = latents.astype(full_type)
    cross_normed_out, cross_normed, cross_inv = norm_forward(initial, cross_gain)
    query_part, cross_rows = project_cols(
        cross_normed_out.astype(low_type), cross_query, FORWARD_FIRST
    )
    query_all = query_feats(query_part.astype(low_type))
    input_full = inputs.astype(full_type)
    input_center = input_full - jnp.mean(input_full, axis=-1, keepdims=True)
    input_inv = lax.rsqrt(jnp.mean(input_center * input_center, axis=-1) + EPS)
    input_normed = input_center * input_inv[..., None]
    input_low = (input_normed * input_gain).astype(low_type)

    def project_keys(rows):
        key_block = jnp.dot(rows, cross_key, preferred_element_type=full_type).astype(low_type)
        value_block = jnp.dot(rows, cross_value, preferred_element_type=full_type).astype(low_type)
        return (key_block, value_block)

    keys_all, values_all = lax.map(project_keys, input_low)
    scores = (
        jnp.einsum("sqd,skd->sqk", query_all, keys_all, preferred_element_type=full_type)
        * cross_scale
    )
    local_top = jnp.max(jnp.where(cross_mask, scores, NEGATIVE), axis=-1)
    local_total = jnp.sum(
        jnp.where(cross_mask, jnp.exp(scores - local_top[..., None]), 0.0), axis=-1
    )
    merged_top, merged_total = joined_2((local_top, local_total), "col", merge_softmax)
    cross_lse = merged_top + jnp.log(merged_total)
    cross_chances = jnp.where(cross_mask, jnp.exp(scores - cross_lse[..., None]), 0.0).astype(
        low_type
    )
    attended_part = jnp.einsum(
        "sqk,skd->sqd", cross_chances, values_all, preferred_element_type=full_type
    )
    attended_all = lax.psum(attended_part.astype(jnp.bfloat16), "col").astype(jnp.float32)
    attended_here = lax.dynamic_slice_in_dim(
        attended_all, col_at * column_width_count, column_width_count, 2
    )
    cross_branch, attended_rows = project_rows(
        attended_here.astype(low_type), cross_out, FORWARD_SECOND
    )
    after_cross = initial + cross_branch
    after_first, first_saved = feed_forward(after_cross, first_gain, first_expand, first_shrink)
    self_normed_out, self_normed, self_inv = norm_forward(after_first, self_gain)
    joined = jnp.concatenate([self_query, self_key, self_value], axis=1)
    projected, self_rows = project_cols(self_normed_out.astype(low_type), joined, FORWARD_FIRST)
    projected_low = projected.astype(low_type)
    pair_all = row_rows(projected_low[..., column_width_count:])
    heads_q = projected_low[..., :column_width_count].reshape(seqs, rows_here, heads_here, HEAD)
    heads_k = pair_all[..., :column_width_count].reshape(seqs, total_rows, heads_here, HEAD)
    heads_v = pair_all[..., column_width_count:].reshape(seqs, total_rows, heads_here, HEAD)
    self_scores = (
        jnp.einsum("sqhd,skhd->shqk", heads_q, heads_k, preferred_element_type=full_type)
        * self_scale
    )
    self_top = jnp.max(jnp.where(latent_attend_mask, self_scores, NEGATIVE), axis=-1)
    self_total = jnp.sum(
        jnp.where(latent_attend_mask, jnp.exp(self_scores - self_top[..., None]), 0.0), axis=-1
    )
    self_lse = self_top + jnp.log(self_total)
    self_chances = jnp.where(
        latent_attend_mask, jnp.exp(self_scores - self_lse[..., None]), 0.0
    ).astype(low_type)
    self_mixed = jnp.einsum(
        "shqk,skhd->sqhd", self_chances, heads_v, preferred_element_type=full_type
    )
    self_branch, mixed_rows = project_rows(
        self_mixed.reshape(seqs, rows_here, column_width_count).astype(low_type),
        self_out,
        FORWARD_SECOND,
    )
    after_self = after_first + self_branch
    final_state, second_saved = feed_forward(after_self, second_gain, second_expand, second_shrink)
    result = final_state.astype(low_type)
    grad_state = cotangent.astype(full_type)
    grad_state, grad_second_gain, grad_second_expand, grad_second_shrink = feed_backward(
        grad_state, second_saved, second_gain, second_expand, second_shrink
    )
    grad_mixed, self_branch_rows = project_cols(
        grad_state.astype(low_type), self_out, BACKWARD_SECOND
    )
    grad_self_out = weight_grad(GRADIENT_SECOND, mixed_rows, self_branch_rows)
    grad_mixed_low = grad_mixed.astype(low_type).reshape(seqs, rows_here, heads_here, HEAD)
    self_delta = jnp.transpose(
        jnp.sum(grad_mixed_low.astype(full_type) * self_mixed, axis=-1), (0, 2, 1)
    )
    again_scores = (
        jnp.einsum("sqhd,skhd->shqk", heads_q, heads_k, preferred_element_type=full_type)
        * self_scale
    )
    again_chances = jnp.where(latent_attend_mask, jnp.exp(again_scores - self_lse[..., None]), 0.0)
    grad_self_chances = jnp.einsum(
        "sqhd,skhd->shqk", grad_mixed_low, heads_v, preferred_element_type=full_type
    )
    grad_self_scores = (again_chances * (grad_self_chances - self_delta[..., None])).astype(
        low_type
    )
    grad_heads_q = (
        jnp.einsum("shqk,skhd->sqhd", grad_self_scores, heads_k, preferred_element_type=full_type)
        * self_scale
    )
    grad_heads_k = (
        jnp.einsum("shqk,sqhd->skhd", grad_self_scores, heads_q, preferred_element_type=full_type)
        * self_scale
    )
    grad_heads_v = jnp.einsum(
        "shqk,sqhd->skhd",
        again_chances.astype(low_type),
        grad_mixed_low,
        preferred_element_type=full_type,
    )
    pair_grad = row_reduce(
        jnp.concatenate(
            [
                grad_heads_k.reshape(seqs, total_rows, column_width_count),
                grad_heads_v.reshape(seqs, total_rows, column_width_count),
            ],
            axis=-1,
        )
    )
    joined_grad = jnp.concatenate(
        [grad_heads_q.reshape(seqs, rows_here, column_width_count), pair_grad], axis=-1
    ).astype(low_type)
    grad_self_in, joined_rows = project_rows(joined_grad, joined, BACKWARD_FIRST)
    grad_joined = weight_grad(GRADIENT_FIRST, self_rows, joined_rows)
    grad_self_normed, grad_self_gain = norm_backward(grad_self_in, self_gain, self_normed, self_inv)
    grad_state = grad_state + grad_self_normed
    grad_state, grad_first_gain, grad_first_expand, grad_first_shrink = feed_backward(
        grad_state, first_saved, first_gain, first_expand, first_shrink
    )
    grad_attended, cross_branch_rows = project_cols(
        grad_state.astype(low_type), cross_out, BACKWARD_SECOND
    )
    grad_cross_out = weight_grad(GRADIENT_SECOND, attended_rows, cross_branch_rows)
    grad_attended_all = query_feats(grad_attended.astype(low_type))
    cross_delta = jnp.sum(grad_attended_all.astype(full_type) * attended_all, axis=-1)

    def cross_back_one(carry, item):
        query_one, keys_one, values_one, grad_one, lse_one, delta_one, mask_one, normed_one = item
        scores_one = (
            jnp.einsum("qd,kd->qk", query_one, keys_one, preferred_element_type=full_type)
            * cross_scale
        )
        chances_one = jnp.where(mask_one, jnp.exp(scores_one - lse_one[:, None]), 0.0)
        grad_chances = jnp.einsum(
            "qd,kd->qk", grad_one, values_one, preferred_element_type=full_type
        )
        grad_scores = (chances_one * (grad_chances - delta_one[:, None])).astype(low_type)
        grad_query = (
            jnp.einsum("qk,kd->qd", grad_scores, keys_one, preferred_element_type=full_type)
            * cross_scale
        )
        grad_keys = (
            jnp.einsum("qk,qd->kd", grad_scores, query_one, preferred_element_type=full_type)
            * cross_scale
        )
        grad_values = jnp.einsum(
            "qk,qd->kd", chances_one.astype(low_type), grad_one, preferred_element_type=full_type
        )
        grad_normed = split_einsum("kd,cd->kc", grad_keys, cross_key, True) + split_einsum(
            "kd,cd->kc", grad_values, cross_value, True
        )
        key_sum = carry[0] + split_einsum("kc,kd->cd", grad_keys, normed_one, False)
        value_sum = carry[1] + split_einsum("kc,kd->cd", grad_values, normed_one, False)
        return ((key_sum, value_sum), (grad_query, grad_normed))

    empty = jnp.zeros(cross_key.shape, full_type)
    (grad_key_sum, grad_value_sum), (grad_query_all, grad_input_part) = lax.scan(
        cross_back_one,
        (empty, empty),
        (
            query_all,
            keys_all,
            values_all,
            grad_attended_all,
            cross_lse,
            cross_delta,
            cross_mask,
            input_low,
        ),
    )
    grad_query_here = query_grads(grad_query_all).astype(low_type)
    grad_cross_in, query_rows = project_rows(grad_query_here, cross_query, BACKWARD_FIRST)
    grad_cross_query = weight_grad(GRADIENT_FIRST, cross_rows, query_rows)
    grad_cross_normed, grad_cross_gain = norm_backward(
        grad_cross_in, cross_gain, cross_normed, cross_inv
    )
    grad_latents = grad_state + grad_cross_normed
    input_gain_part = jnp.sum(grad_input_part * input_normed, axis=(0, 1))
    summed = lax.psum(grad_input_part.astype(jnp.bfloat16), "row").astype(jnp.float32)
    grad_inputs = input_back(summed, input_normed, input_inv, input_gain).astype(low_type)
    grid = (
        lax.psum(grad_cross_query.astype(jnp.bfloat16), "dp").astype(jnp.float32),
        lax.psum(grad_cross_out.astype(jnp.bfloat16), "dp").astype(jnp.float32),
        lax.psum(grad_first_expand.astype(jnp.bfloat16), "dp").astype(jnp.float32),
        lax.psum(grad_first_shrink.astype(jnp.bfloat16), "dp").astype(jnp.float32),
        lax.psum(grad_joined.astype(jnp.bfloat16), "dp").astype(jnp.float32),
        lax.psum(grad_self_out.astype(jnp.bfloat16), "dp").astype(jnp.float32),
        lax.psum(grad_second_expand.astype(jnp.bfloat16), "dp").astype(jnp.float32),
        lax.psum(grad_second_shrink.astype(jnp.bfloat16), "dp").astype(jnp.float32),
    )
    gains_local = jnp.stack([grad_cross_gain, grad_first_gain, grad_self_gain, grad_second_gain])
    padded = lax.dynamic_update_slice(
        jnp.zeros((4, width_row * lax.axis_size("row")), full_type),
        gains_local,
        (jnp.int32(0), row_at * width_row),
    )
    shared = lax.psum((grad_key_sum, grad_value_sum, padded, input_gain_part), ("row", "col", "dp"))
    gains_all = lax.dynamic_slice_in_dim(shared[2], row_at * width_row, width_row, 1)
    joined_sum = grid[4]
    return (
        result,
        grad_latents,
        grad_inputs,
        gains_all[0],
        shared[3],
        grid[0],
        shared[0],
        shared[1],
        grid[1],
        gains_all[1],
        grid[2],
        grid[3],
        gains_all[2],
        joined_sum[:, :column_width_count],
        joined_sum[:, column_width_count : 2 * column_width_count],
        joined_sum[:, 2 * column_width_count :],
        grid[5],
        gains_all[3],
        grid[6],
        grid[7],
    )


NEG = -1e30
WIDE = 256
BLOCK = 128


def col_step(flip):
    return tuple((c, c ^ flip) for c in range(4))


ROW_SWAP = ((0, 1), (1, 0))
BOTH_SWAP = tuple((r * 4 + c, (1 - r) * 4 + (c ^ 2)) for r in range(2) for c in range(4))
SEQ_NEAR = ((0, 1), (1, 0), (2, 3), (3, 2))
SEQ_FAR = ((0, 2), (2, 0), (1, 3), (3, 1))
GROUP = ("col", "row")


def swap_row(value):
    return lax.ppermute(value, "row", ROW_SWAP)


def swap_chip(value):
    return lax.ppermute(value, "col", col_step(2))


def swap_core(value):
    return lax.ppermute(value, "col", col_step(1))


def swap_both(value):
    return lax.ppermute(value, ("row", "col"), BOTH_SWAP)


def gather_eight(value):
    near = [value, swap_row(value), swap_chip(value), swap_both(value)]
    return near + [swap_core(part) for part in near]


def exchange(value):
    return lax.all_to_all(value, GROUP, 0, 0, tiled=True)


def hold(values, *others):
    return lax.optimization_barrier(tuple(values) + others)[: len(values)]


def after(value, *others):
    return lax.optimization_barrier((value,) + others)[0]


class Any:
    def __init__(self, value):
        self.value = value


class Small:
    def __init__(self, value):
        self.value = value


def kernel(body, outs, *args, scratch=()):
    spaces = {Any: pl.ANY, Small: pltpu.SMEM}
    specs = [pl.BlockSpec(memory_space=spaces.get(type(arg), pltpu.VMEM)) for arg in args]
    values = [arg.value if type(arg) in spaces else arg for arg in args]
    return pl.pallas_call(
        body,
        out_shape=tuple(jax.ShapeDtypeStruct(shape, kind) for shape, kind in outs),
        in_specs=specs,
        out_specs=tuple(pl.BlockSpec(memory_space=pltpu.VMEM) for _ in outs),
        scratch_shapes=list(scratch),
        compiler_params=pltpu.CompilerParams(vmem_limit_bytes=56 * 1024 * 1024),
    )(*values)


def from_plane(half, *others):
    half = after(half, *others)
    return [swap_row(half), swap_chip(half), swap_both(half)]


def from_next(parts, *others):
    parts = lax.optimization_barrier(tuple(parts) + others)[: len(parts)]
    return [lax.ppermute(part, "dp", SEQ_NEAR) for part in parts]


def from_core(parts, *others):
    parts = lax.optimization_barrier(tuple(parts) + others)[: len(parts)]
    return [swap_core(part) for part in parts]


def weight_buffer(count):
    return [pltpu.VMEM((8, 2, count * WIDE, WIDE), jnp.bfloat16), pltpu.SemaphoreType.DMA((16,))]


def load_weights(scalars, blocks, buffer, sems, first):
    height = buffer.shape[2]
    rows = pl.ds(first * WIDE, height)
    plane = scalars[4]
    copies = []
    for core in range(2):
        for half in range(2):
            copies.append((blocks[core].at[half, rows, :], block_of(scalars, 0, core), half))
    for k, block in enumerate(blocks[2:]):
        core, other, step = k // 6, k // 3 % 2, k % 3 + 1
        half = 1 - plane if other else plane
        copies.append((block.at[rows, :], block_of(scalars, step, core), half))
    copies = [
        pltpu.make_async_copy(source, buffer.at[block, half], sems.at[k])
        for k, (source, block, half) in enumerate(copies)
    ]
    for copy in copies:
        copy.start()
    return copies


def load_plain(scalars, blocks, buffer, sems):
    copies = [
        pltpu.make_async_copy(
            block, buffer.at[block_of(scalars, j % 4, j // 4)], sems.at[j]
        )
        for j, block in enumerate(blocks)
    ]
    for copy in copies:
        copy.start()
    return copies


def plain_buffer():
    return [pltpu.VMEM((8, 512, WIDE), jnp.bfloat16), pltpu.SemaphoreType.DMA((8,))]


def wait_all(copies):
    for copy in copies:
        copy.wait()


def mm(a, b):
    return lax.dot_general(a, b, (((1,), (0,)), ((), ())), preferred_element_type=jnp.float32)


def mt(a, b):
    return lax.dot_general(a, b, (((1,), (1,)), ((), ())), preferred_element_type=jnp.float32)


def low(v):
    return v.astype(jnp.bfloat16)


def full(v):
    return v.astype(jnp.float32)


def norm_parts(value):
    width = value.shape[-1]
    center = jnp.sum(value, axis=-1, keepdims=True) / width
    shifted = value - center
    spread = jnp.sum(shifted * shifted, axis=-1, keepdims=True) / width
    inv = lax.rsqrt(spread + EPS)
    return shifted * inv, inv


def norm_back(grad, gain, normed, inv):
    width = grad.shape[-1]
    scaled = grad * gain
    first = jnp.sum(scaled, axis=-1, keepdims=True) / width
    second = jnp.sum(scaled * normed, axis=-1, keepdims=True) / width
    return inv * (scaled - first - normed * second), jnp.sum(grad * normed, axis=0, keepdims=True)


def phi(value):
    return 0.5 * (1.0 + lax.erf(value * (1.0 / math.sqrt(2.0))))


def gelu_value(value):
    return value * phi(value)


def gelu_slope(value):
    return phi(value) + value * jnp.exp(value * value * -0.5) * (1.0 / math.sqrt(2.0 * math.pi))


def three(value):
    first = low(value)
    rest = value - full(first)
    second = low(rest)
    return full(first), full(second), rest - full(second)


def block_of(scalars, step, core):
    return scalars[0] ^ (4 * (step // 2) + 2 * core + step % 2)


def rows_of(count, lanes):
    return lax.broadcasted_iota(jnp.int32, (count, lanes), 0)


def add_kernel(parts, total):
    acc = full(parts[0])
    for b in range(1, parts.shape[0]):
        acc = acc + full(parts[b])
    total[...] = low(acc)


def input_kernel(scalars, inputs, gain, plain, turned, rows, sem):
    count, channels = rows.shape
    at = pl.multiple_of(scalars[1] * count, count)
    copy = pltpu.make_async_copy(inputs.at[pl.ds(at, count), :], rows, sem)
    copy.start()
    plain[...] = jnp.zeros_like(plain)
    turned[...] = jnp.zeros_like(turned)
    copy.wait()
    normed, _ = norm_parts(full(rows[...]))
    result = normed * gain[...]
    plain[:, 0:channels] = low(result)
    turned[0:channels, :] = low(result.T)


def pack_kernel(scalars, query, key, value, *rest):
    weights, (mine, theirs, first, first_half, second, second_half) = rest[:6], rest[7:]
    for k, weight in enumerate((query, key, value)):
        for place, row in ((mine, scalars[1]), (theirs, 1 - scalars[1])):
            at = pl.multiple_of(row * HEAD, HEAD)
            place[:, k * HEAD : (k + 1) * HEAD] = weight[:, pl.ds(at, HEAD)]
    for k, weight in enumerate(weights):
        whole, half = ((first, first_half), (second, second_half))[k // 3]
        rows = slice(k % 3 * WIDE, (k % 3 + 1) * WIDE)
        at = pl.multiple_of(scalars[4] * WIDE, WIDE)
        if weight.shape[0] == WIDE:
            whole[0, rows, :] = weight[:, :WIDE]
            whole[1, rows, :] = weight[:, WIDE:]
            half[rows, :] = weight[:, pl.ds(at, WIDE)]
        else:
            whole[0, rows, :] = weight[:WIDE, :]
            whole[1, rows, :] = weight[WIDE:, :]
            half[rows, :] = weight[pl.ds(at, WIDE), :]


def query_kernel(
    scalars, latents, other, gains, key, *rest
):
    blocks, (state, normed_in, folded, query, wide, buffer, sems) = rest[1:9], rest[9:]
    copies = load_plain(scalars, blocks, buffer, sems)
    row = scalars[1]
    rows = pl.multiple_of(row * BLOCK, BLOCK)
    mine = pl.multiple_of(row * 512, 512)
    theirs = pl.multiple_of((1 - row) * 512, 512)
    state[:, pl.ds(mine, 512)] = latents[pl.ds(rows, BLOCK), :]
    state[:, pl.ds(theirs, 512)] = other[...]
    value, _ = norm_parts(full(state[...]))
    normed_in[...] = low(value * gains[0:1, :])
    channels = key.shape[0]
    folded[...] = jnp.zeros_like(folded)
    wait_all(copies)
    for r in range(2):
        acc = None
        for c in range(4):
            part = mt(key[:, c * WIDE : (c + 1) * WIDE], buffer[2 * c + r])
            acc = part if acc is None else acc + part
        folded[0:channels, r * 512 : (r + 1) * 512] = low(acc)
    query[...] = low(mt(folded[...], normed_in[...]) * (1.0 / math.sqrt(D)))


BULK = 14


def fold_out_kernel(scalars, value, *rest):
    blocks, (folded, buffer, sems) = rest[:BULK], rest[BULK:]
    copies = load_weights(scalars, blocks, buffer, sems, 0)
    channels = value.shape[0]
    folded[...] = jnp.zeros_like(folded)
    wait_all(copies)
    folded[0:channels, :] = low(shrink_tiles(value[...], buffer, 0))


def cross_kernel(scalars, limits, plain, turned, *rest, channels):
    blocks, (queries, result) = rest[:8], rest[8:]
    for j, block in enumerate(blocks):
        queries[block_of(scalars, j % 4, j // 4)] = block[...]
    base = scalars[3]
    count, padded = plain.shape

    def pair(i, carry):
        query = jnp.concatenate([queries[2 * i], queries[2 * i + 1]], axis=1)
        limit = jnp.concatenate([limits[2 * i], limits[2 * i + 1]], axis=1)
        scores = mm(plain[...], query)
        keys = rows_of(count, 2 * BLOCK) + base
        mask = keys < limit
        top = jnp.max(jnp.where(mask, scores, NEG), axis=0, keepdims=True)
        weights = jnp.where(mask, jnp.exp(scores - top), 0.0)
        total = jnp.sum(weights, axis=0, keepdims=True)
        mixed = mm(turned[...], low(weights))
        some = total > 0.0
        mixed = mixed * jnp.where(some, 1.0 / jnp.where(some, total, 1.0), 0.0)
        lse = jnp.where(some, top + jnp.log(jnp.where(some, total, 1.0)), NEG)
        index = rows_of(padded, 2 * BLOCK)
        for k, part in enumerate(three(lse)):
            mixed = jnp.where(index == channels + k, part, mixed)
        mixed = low(mixed)
        result[2 * i] = mixed[:, :BLOCK]
        result[2 * i + 1] = mixed[:, BLOCK:]
        return carry

    lax.fori_loop(0, 4, pair, 0)


def tile_of(packed, c, r, half, at):
    return packed[2 * c + r, half, at * WIDE : (at + 1) * WIDE, :]


def part_of(value, index):
    return value[:, index * WIDE : (index + 1) * WIDE]


def summed(parts):
    acc = parts[0]
    for part in parts[1:]:
        acc = acc + part
    return acc


def expand_tiles(value, packed, at):
    return jnp.concatenate(
        [
            summed(
                [
                    mm(part_of(value, 2 * r + h), tile_of(packed, c, r, h, at))
                    for r in range(2)
                    for h in range(2)
                ]
            )
            for c in range(4)
        ],
        axis=1,
    )


def shrink_tiles(value, packed, at):
    return jnp.concatenate(
        [
            summed([mm(part_of(value, c), tile_of(packed, c, r, h, at)) for c in range(4)])
            for r in range(2)
            for h in range(2)
        ],
        axis=1,
    )


def expand_back(value, packed, at):
    return jnp.concatenate(
        [
            summed([mt(part_of(value, c), tile_of(packed, c, r, h, at)) for c in range(4)])
            for r in range(2)
            for h in range(2)
        ],
        axis=1,
    )


def shrink_back(value, packed, at):
    return jnp.concatenate(
        [
            summed(
                [
                    mt(part_of(value, 2 * r + h), tile_of(packed, c, r, h, at))
                    for r in range(2)
                    for h in range(2)
                ]
            )
            for c in range(4)
        ],
        axis=1,
    )


def merge_kernel(scalars, parts, latents, folded_out, gains, *rest, channels):
    blocks, rest = rest[:BULK], rest[BULK:]
    mixed_out, lse_out, after_cross, hidden, upward, active, after_first, self_in = rest[:8]
    packed, sems = rest[8:]
    copies = load_weights(scalars, blocks, packed, sems, 1)
    lses = []
    for d in range(8):
        rows = full(parts[d, channels : channels + 3, :])
        lses.append(rows[0:1] + rows[1:2] + rows[2:3])
    top = lses[0]
    for item in lses[1:]:
        top = jnp.maximum(top, item)
    total = jnp.zeros_like(top)
    mixed = jnp.zeros(parts.shape[1:], jnp.float32)
    for d in range(8):
        share = jnp.exp(lses[d] - top)
        total = total + share
        mixed = mixed + full(parts[d]) * share
    mixed = low(mixed / total)
    mixed_out[...] = mixed
    lse_out[...] = top + jnp.log(total)
    branch = mm(low(full(mixed).T), folded_out[...])
    state = full(latents[...]) + branch
    after_cross[...] = state
    normed, _ = norm_parts(state)
    hid = low(normed * gains[1:2, :])
    hidden[...] = hid
    wait_all(copies)
    up = expand_tiles(hid, packed, 0)
    upward[...] = up
    act = low(gelu_value(up))
    active[...] = act
    state = state + shrink_tiles(act, packed, 1)
    after_first[...] = state
    normed, _ = norm_parts(state)
    self_in[...] = low(normed * gains[2:3, :])


def attend_kernel(scalars, mine, theirs, limits, places, *rest):
    blocks, (rows_out, weights, qkv_out, mixed_out, lse_out, sent) = rest[:8], rest[8:]
    row = scalars[1]
    weights[pl.ds(pl.multiple_of(row * 512, 512), 512), :] = mine[...]
    weights[pl.ds(pl.multiple_of((1 - row) * 512, 512), 512), :] = theirs[...]
    for j, block in enumerate(blocks):
        at = pl.multiple_of(block_of(scalars, j % 4, j // 4) * BLOCK, BLOCK)
        rows_out[pl.ds(at, BLOCK), :] = block[...]
    qkv_out[...] = low(mm(rows_out[...], weights[...]))
    scale = 1.0 / math.sqrt(HEAD)
    turned = low(full(qkv_out[:, 2 * HEAD :]).T)

    def pair(i, carry):
        at = pl.multiple_of(i * WIDE, WIDE)
        query = qkv_out[pl.ds(at, WIDE), 0:HEAD]
        scores = mt(qkv_out[:, HEAD : 2 * HEAD], query) * scale
        limit = jnp.concatenate([limits[2 * i], limits[2 * i + 1]], axis=1)
        mask = places[...] < limit
        top = jnp.max(jnp.where(mask, scores, NEG), axis=0, keepdims=True)
        share = jnp.where(mask, jnp.exp(scores - top), 0.0)
        total = jnp.sum(share, axis=0, keepdims=True)
        mixed = mm(turned, low(share)) / total
        mixed_out[:, pl.ds(at, WIDE)] = mixed
        lse_out[:, pl.ds(at, WIDE)] = top + jnp.log(total)
        lower = low(mixed)
        sent[2 * i] = lower[:, :BLOCK]
        sent[2 * i + 1] = lower[:, BLOCK:]
        return carry

    lax.fori_loop(0, 4, pair, 0)


def split_halves(scalars, values, keep, give):
    row = scalars[1]
    for k, value in enumerate(values):
        low_half, high_half = value[:, :512], value[:, 512:]
        keep[k] = jnp.where(row == 0, low_half, high_half)
        give[k] = jnp.where(row == 0, high_half, low_half)


def split_quarters(scalars, values, quarters):
    for k, value in enumerate(values):
        for c in range(4):
            quarters[scalars[2] ^ c, k] = part_of(value, c)


def second_kernel(scalars, parts, after_first, cotangent, gains, early_hidden, early_active, *rest):
    blocks, rest = rest[:BULK], rest[BULK:]
    out, keep, give, quarters, grad_gain, state_grad, sent = rest[:7]
    packed, sems = rest[7:]
    gain = gains[3:4, :]
    copies = load_weights(scalars, blocks, packed, sems, 0)
    att = low(jnp.concatenate([full(parts[h]).T for h in range(8)], axis=1))
    wait_all(copies)
    state = after_first[...] + shrink_tiles(att, packed, 0)
    normed, inv = norm_parts(state)
    hid = low(normed * gain)
    up = expand_tiles(hid, packed, 1)
    act = low(gelu_value(up))
    out[...] = low(state + shrink_tiles(act, packed, 2))
    grad = cotangent[...]
    gu = low(shrink_back(grad, packed, 2) * gelu_slope(up))
    back, grad_gain[...] = norm_back(expand_back(gu, packed, 1), gain, normed, inv)
    total = full(grad) + back
    state_grad[...] = total
    lower = low(total)
    grad_att = shrink_back(lower, packed, 0)
    for h in range(8):
        sent[h] = low(grad_att[:, h * BLOCK : (h + 1) * BLOCK].T)
    split_halves(scalars, (hid, grad, lower, early_hidden[...]), keep, give)
    split_quarters(scalars, (gu, act, att, early_active[...]), quarters)


def put_chunk(scalars, keep, give, index, value):
    here = scalars[4] == index // 2
    at = scalars[5] ^ (index % 2)

    @pl.when(here)
    def _():
        keep[at] = value

    @pl.when(jnp.logical_not(here))
    def _():
        give[at] = value


def read_chunk(scalars, mine, theirs, index):
    at = scalars[5] ^ (index % 2)
    return jnp.where(scalars[4] == index // 2, full(mine[at]), full(theirs[at]))


def columns(value, index):
    return value[:, index * BLOCK : (index + 1) * BLOCK]


def row_block(value, index):
    return value[index * BLOCK : (index + 1) * BLOCK, :]


def weight_kernel(scalars, *refs):
    halves, quarters, rest = refs[:8], refs[8:16], refs[16:]
    keep, give, halves_turned, quarters_all, quarters_turned = rest
    for k in range(3):
        for j in range(8):
            at = slice(j * BLOCK, (j + 1) * BLOCK)
            if k == 0:
                halves_turned[:, at] = low(full(halves[j][k]).T)
                quarters_all[at, :] = quarters[j][k]
            else:
                quarters_turned[k - 1, :, at] = low(full(quarters[j][k]).T)
    expand = low(mm(halves_turned[...], quarters_all[...]))
    shrinks = [
        low(summed([
            mm(quarters_turned[k - 1, :, j * BLOCK : (j + 1) * BLOCK], halves[j][k])
            for j in range(8)
        ]))
        for k in (1, 2)
    ]
    for t in range(4):
        parts = jnp.concatenate([columns(value, t) for value in shrinks], axis=1)
        put_chunk(scalars, keep, give, t, jnp.concatenate([row_block(expand, t), parts], axis=0))


def weight_out_kernel(scalars, mine, theirs, expand, first_shrink, second_shrink):
    for t in range(4):
        chunk = read_chunk(scalars, mine, theirs, t)
        at = slice(t * BLOCK, (t + 1) * BLOCK)
        expand[at, :] = chunk[:BLOCK]
        first_shrink[:, at] = chunk[BLOCK:, :BLOCK]
        second_shrink[:, at] = chunk[BLOCK:, BLOCK:]


def last_weight_kernel(scalars, *refs):
    early_halves, early_quarters, halves, quarters = refs[:8], refs[8:16], refs[16:24], refs[24:32]
    keep, give, halves_turned, quarters_all, quarters_turned = refs[32:]
    for j in range(8):
        at = slice(j * BLOCK, (j + 1) * BLOCK)
        halves_turned[:, at] = low(full(early_halves[j][3]).T)
        quarters_all[at, :] = quarters[j][0]
        quarters_turned[:, at] = low(full(early_quarters[j][3]).T)
    expand = low(mm(halves_turned[...], quarters_all[...]))
    shrink = low(summed([
        mm(quarters_turned[:, j * BLOCK : (j + 1) * BLOCK], halves[j][0]) for j in range(8)
    ]))
    for t in range(4):
        part = columns(shrink, t)
        parts = jnp.concatenate([part[:BLOCK], part[BLOCK:]], axis=1)
        put_chunk(scalars, keep, give, t, jnp.concatenate([row_block(expand, t), parts], axis=0))


def last_weight_out_kernel(scalars, mine, theirs, expand, shrink):
    for t in range(4):
        chunk = read_chunk(scalars, mine, theirs, t)
        at = slice(t * BLOCK, (t + 1) * BLOCK)
        expand[at, :] = chunk[:BLOCK]
        shrink[:BLOCK, at] = chunk[BLOCK:, :BLOCK]
        shrink[BLOCK:, at] = chunk[BLOCK:, BLOCK:]


def head_weight_kernel(scalars, rows, grads, keep, give):
    turned = low(full(grads[...]).T)
    total = mm(turned, rows[...]).T
    row = scalars[1]
    mine = low(jnp.where(row == 0, total[:512], total[512:]))
    theirs = low(jnp.where(row == 0, total[512:], total[:512]))
    for t in range(4):
        put_chunk(
            scalars, keep, give, t,
            jnp.concatenate([row_block(mine, t), row_block(theirs, t)], axis=1),
        )


def head_out_kernel(scalars, mine, theirs, keep, give):
    width = keep.shape[1]
    for t in range(4):
        chunk = low(read_chunk(scalars, mine, theirs, t))
        at = slice(t * BLOCK, (t + 1) * BLOCK)
        keep[at, :] = chunk[:, :width]
        give[at, :] = chunk[:, width:]


def attend_back_kernel(
    scalars, parts, qkv, mixed, lse, weights, limits, places, grads, sent
):
    scale = 1.0 / math.sqrt(HEAD)
    keys_turned = low(full(qkv[:, HEAD : 2 * HEAD]).T)

    def pair(i, carry):
        grad_k, grad_v = carry
        at = pl.multiple_of(i * WIDE, WIDE)
        query = qkv[pl.ds(at, WIDE), 0:HEAD]
        grad_out = jnp.concatenate([parts[2 * i], parts[2 * i + 1]], axis=1)
        delta = jnp.sum(full(grad_out) * mixed[:, pl.ds(at, WIDE)], axis=0, keepdims=True)
        scores = mt(qkv[:, HEAD : 2 * HEAD], query) * scale
        limit = jnp.concatenate([limits[2 * i], limits[2 * i + 1]], axis=1)
        mask = places[...] < limit
        share = jnp.where(mask, jnp.exp(scores - lse[:, pl.ds(at, WIDE)]), 0.0)
        grad_share = mm(qkv[:, 2 * HEAD :], grad_out)
        grad_scores = low(share * (grad_share - delta))
        grad_k = grad_k + mm(grad_scores, query)
        grad_v = grad_v + mt(low(share), grad_out)
        grad_q = mm(keys_turned, grad_scores) * scale
        grads[pl.ds(at, WIDE), 0:HEAD] = low(grad_q.T)
        return grad_k, grad_v

    zero = jnp.zeros((qkv.shape[0], HEAD), jnp.float32)
    grad_k, grad_v = lax.fori_loop(0, 4, pair, (zero, zero))
    grads[:, HEAD : 2 * HEAD] = low(grad_k * scale)
    grads[:, 2 * HEAD :] = low(grad_v)
    for step in range(4):
        for core in range(2):
            at = pl.multiple_of(block_of(scalars, step, core) * BLOCK, BLOCK)
            sent[core, step] = low(mt(grads[pl.ds(at, BLOCK), :], weights[...]))


def first_back_kernel(
    scalars, own, by_row, by_chip, by_both, state_grad, after_first, after_cross, upward, gains,
    folded_out, mixed, lse, *rest, channels
):
    blocks, rest = rest[:BULK], rest[BULK:]
    gain_grads, keep, give, quarters, cross_grad, value_part, sent = rest[:7]
    packed, sems = rest[7:]
    copies = load_weights(scalars, blocks, packed, sems, 1)
    grad_in = full(own[...]) + full(by_row[...]) + full(by_chip[...]) + full(by_both[...])
    normed, inv = norm_parts(after_first[...])
    back, self_gain = norm_back(grad_in, gains[2:3, :], normed, inv)
    grad = state_grad[...] + back
    lower = low(grad)
    wait_all(copies)
    gu = low(shrink_back(lower, packed, 1) * gelu_slope(upward[...]))
    split_halves(scalars, (lower,), keep, give)
    split_quarters(scalars, (gu,), quarters)
    grad_hid = expand_back(gu, packed, 0)
    normed, inv = norm_parts(after_cross[...])
    back, first_gain = norm_back(grad_hid, gains[1:2, :], normed, inv)
    gain_grads[0:1, :] = first_gain
    gain_grads[1:2, :] = self_gain
    grad = grad + back
    cross_grad[...] = grad
    lower = low(grad)
    value_part[...] = low(mm(mixed[...], lower))
    grad_mixed = mt(folded_out[...], lower)
    padded = grad_mixed.shape[0]
    index = rows_of(padded, BLOCK)
    grad_mixed = jnp.where(index < channels, grad_mixed, 0.0)
    rounded = full(low(grad_mixed))
    delta = jnp.sum(rounded * full(mixed[...]), axis=0, keepdims=True)
    for k, part in enumerate(three(lse[...]) + three(delta)):
        grad_mixed = jnp.where(index == channels + k, part, grad_mixed)
    sent[...] = low(grad_mixed)


def cross_back_kernel(scalars, queries, limits, plain, turned, inputs, gain, *rest, channels):
    blocks, (grad_rows, grad_gain, sent, grads, total, rows, sem) = rest[:8], rest[8:]
    at = pl.multiple_of(scalars[1] * rows.shape[0], rows.shape[0])
    copy = pltpu.make_async_copy(inputs.at[pl.ds(at, rows.shape[0]), :], rows, sem)
    copy.start()
    for j, block in enumerate(blocks):
        grads[block_of(scalars, j % 4, j // 4)] = block[...]
    base = scalars[3]
    count, padded = plain.shape
    total[...] = jnp.zeros_like(total)

    def pair(i, carry):
        query = jnp.concatenate([queries[2 * i], queries[2 * i + 1]], axis=1)
        grad_mixed = jnp.concatenate([grads[2 * i], grads[2 * i + 1]], axis=1)
        extra = full(grad_mixed[channels : channels + 6, :])
        lse = extra[0:1] + extra[1:2] + extra[2:3]
        delta = extra[3:4] + extra[4:5] + extra[5:6]
        limit = jnp.concatenate([limits[2 * i], limits[2 * i + 1]], axis=1)
        mask = rows_of(count, 2 * BLOCK) + base < limit
        scores = mm(plain[...], query)
        share = jnp.where(mask, jnp.exp(scores - lse), 0.0)
        grad_share = mm(plain[...], grad_mixed)
        grad_scores = low(share * (grad_share - delta))
        out = low(mm(turned[...], grad_scores) * (1.0 / math.sqrt(D)))
        sent[2 * i] = out[:, :BLOCK]
        sent[2 * i + 1] = out[:, BLOCK:]
        total[...] += mt(grad_scores, query) + mt(low(share), grad_mixed)
        return carry

    lax.fori_loop(0, 4, pair, 0)
    copy.wait()
    normed, inv = norm_parts(full(rows[...]))
    back, wide = norm_back(total[:, 0:channels], gain[...], normed, inv)
    grad_gain[...] = wide
    grad_rows[...] = low(back)


def last_kernel(
    parts, folded_query, normed_in, latents, gains, cross_grad, value_part, gain_rows,
    grad_latents, sent, *, channels
):
    acc = full(parts[0])
    for d in range(1, 8):
        acc = acc + full(parts[d])
    padded = acc.shape[0]
    index = rows_of(padded, BLOCK)
    acc = jnp.where(index < channels, acc, 0.0)
    grad_query = low(acc)
    grad_in = mm(low(acc.T), folded_query[...])
    normed, inv = norm_parts(full(latents[...]))
    back, cross_gain = norm_back(grad_in, gains[0:1, :], normed, inv)
    grad_latents[...] = cross_grad[...] + back
    part = mm(grad_query, normed_in[...])
    wide = rows_of(padded, part.shape[1])
    rows = [cross_gain] + [gain_rows[k : k + 1, :] for k in range(4)]
    for k, row in enumerate(rows):
        high = low(row)
        part = jnp.where(wide == channels + 2 * k, full(high), part)
        part = jnp.where(wide == channels + 2 * k + 1, row - full(high), part)
    part = low(part)
    for b in range(8):
        sent[b, 0] = part[:, b * BLOCK : (b + 1) * BLOCK]
        sent[b, 1] = value_part[:, b * BLOCK : (b + 1) * BLOCK]


def finish_kernel(scalars, key, value, *rest, channels):
    blocks, query_blocks, rest = rest[:8], rest[8:16], rest[16:]
    out_blocks, rest = rest[:BULK], rest[BULK:]
    grad_query, grad_key, grad_out, grad_value, gain_grads = rest[:5]
    key_sum, value_sum, packed, sems, packed_out, out_sems = rest[5:]
    copies = load_plain(scalars, query_blocks, packed, sems)
    copies += load_weights(scalars, out_blocks, packed_out, out_sems, 0)
    for j, block in enumerate(blocks):
        at = pl.multiple_of(block_of(scalars, j % 4, j // 4) * BLOCK, BLOCK)
        key_sum[:, pl.ds(at, BLOCK)] = block[0]
        value_sum[:, pl.ds(at, BLOCK)] = block[1]
    extra = full(key_sum[channels : channels + 10, :])
    for k in range(5):
        gain_grads[k : k + 1, :] = extra[2 * k : 2 * k + 1] + extra[2 * k + 1 : 2 * k + 2]
    at = pl.multiple_of(scalars[2] * WIDE, WIDE)
    half = pl.multiple_of(scalars[1] * 512, 512)
    turned = full(key_sum[:, pl.ds(half, 512)]).T
    grad_query[...] = mm(low(turned[:, :channels]), key[:, pl.ds(at, WIDE)])
    turned = full(value[:, pl.ds(at, WIDE)]).T
    grad_out[...] = mm(low(turned), value_sum[0:channels, pl.ds(half, 512)])
    wait_all(copies)
    for c in range(4):
        acc = mm(key_sum[:, 0:512], packed[2 * c]) + mm(key_sum[:, 512:1024], packed[2 * c + 1])
        grad_key[:, c * WIDE : (c + 1) * WIDE] = acc[:channels]
    grad_value[...] = shrink_back(value_sum[...], packed_out, 0)[:channels]


def wide_rows(value, row):
    half = value.shape[1] // 2
    keep = lax.dynamic_slice_in_dim(value, row * half, half, 1)
    give = lax.dynamic_slice_in_dim(value, (1 - row) * half, half, 1)
    return keep, give


def swap_near(value):
    return lax.ppermute(value, "dp", SEQ_NEAR)


def swap_far(value):
    return lax.ppermute(value, "dp", SEQ_FAR)


def plus(a, b):
    return low(full(a) + full(b))


def swap_cross(value):
    return lax.ppermute(value, "col", col_step(3))


def spread_halves(keep, give):
    mine = [keep, swap_row(give)]
    mine = mine + [swap_chip(part) for part in mine]
    return mine + [swap_core(part) for part in mine]


def spread_quarters(quarters):
    mine = [quarters[0], swap_chip(quarters[2]), swap_core(quarters[1]), swap_cross(quarters[3])]
    theirs = [swap_row(part) for part in mine]
    return [mine[0], theirs[0], mine[1], theirs[1], mine[2], theirs[2], mine[3], theirs[3]]


def over_planes(parts):
    count = parts.shape[0] // 4
    at = lax.axis_index("dp")
    pieces = parts.reshape(4, count, parts.shape[1])
    total = low(jnp.sum(full(lax.all_to_all(pieces, "dp", 0, 0, tiled=True)), axis=0))
    return lax.all_gather(total, "dp", axis=0, tiled=True)


def in_order(row, own, other, axis):
    return jnp.where(
        row == 0,
        jnp.concatenate([own, other], axis),
        jnp.concatenate([other, own], axis),
    )


def tiles_of(weight):
    return [weight[:, :WIDE], weight[:, WIDE:]]


def fast_device(
    latents, inputs, positions, piece_start, cotangent, cross_gain, input_gain, cross_query,
    cross_key, cross_value, cross_out, first_gain, first_expand, first_shrink, self_gain,
    self_query, self_key, self_value, self_out, second_gain, second_expand, second_shrink,
):
    bf, f32 = jnp.bfloat16, jnp.float32
    row, col = lax.axis_index("row"), lax.axis_index("col")
    chip, core = col // 2, col % 2
    channels = inputs.shape[-1]
    padded = -(-(channels + 11) // 16) * 16
    keys_here = inputs.shape[1] // 2
    base = col * inputs.shape[1] + row * keys_here
    plane = lax.axis_index("dp") % 2
    far_plane = lax.axis_index("dp") // 2
    scalars = jnp.stack([2 * col + row, row, col, base, plane, far_plane]).astype(jnp.int32)
    rows = BLOCK

    def swap_half(block):
        keep = lax.dynamic_slice_in_dim(block, row * rows, rows, 0)
        give = lax.dynamic_slice_in_dim(block, (1 - row) * rows, rows, 0)
        return in_order(row, keep, swap_row(give), 1)

    def swap_back(value):
        keep, give = wide_rows(value, row)
        return in_order(row, keep, swap_row(give), 0)

    small = Small(scalars)
    inputs_here = inputs[0]
    gain_here = input_gain[None]
    gains_here = jnp.stack([cross_gain, first_gain, self_gain, second_gain])
    other_rows = swap_row(
        lax.dynamic_slice_in_dim(latents[0], (1 - row) * rows, rows, 0)
    )
    query_blocks = [cross_query] + from_plane(cross_query)
    gains = in_order(row, gains_here, swap_row(gains_here), 1)
    plain, turned = kernel(
        input_kernel,
        [((keys_here, padded), bf), ((padded, keys_here), bf)],
        small, Any(inputs_here), gain_here,
        scratch=[pltpu.VMEM((keys_here, channels), bf), pltpu.SemaphoreType.DMA(())],
    )
    whole, half = (2, 3 * WIDE, WIDE), (3 * WIDE, WIDE)
    mine, theirs, first_whole, first_half, second_whole, second_half = kernel(
        pack_kernel,
        [((512, 3 * HEAD), bf), ((512, 3 * HEAD), bf), (whole, bf), (half, bf), (whole, bf),
         (half, bf)],
        small, self_query, self_key, self_value, cross_out, first_expand, first_shrink, self_out,
        second_expand, second_shrink, Any(plain),
    )
    first_plane = from_plane(first_half, other_rows, gains)
    limits = view_limits(positions, piece_start)[0].reshape(8, 1, BLOCK)
    places = positions[0][:, None]
    query_blocks = query_blocks + from_core(query_blocks, plain)
    state, normed_in, folded_query, query = kernel(
        query_kernel,
        [((rows, D), bf), ((rows, D), bf), ((padded, D), bf), ((padded, rows), bf)],
        small, latents[0], other_rows, gains, cross_key, Any(plain),
        *[Any(block) for block in query_blocks],
        scratch=[pltpu.VMEM((8, BLOCK), f32)] + plain_buffer(),
    )
    query_parts = gather_eight(query)
    theirs = swap_row(after(theirs, query))
    first_next = from_next(first_plane, query)
    queries, partial_mixed = kernel(
        functools.partial(cross_kernel, channels=channels),
        [((8, padded, BLOCK), bf), ((8, padded, BLOCK), bf)],
        small, limits, plain, turned, *query_parts,
    )
    received = exchange(partial_mixed)
    first_core = from_core([first_whole] + first_plane, partial_mixed)
    second_plane = from_plane(second_half, received)
    first_last = from_core(first_next, received)
    first_blocks = [
        Any(block)
        for block in [first_whole, first_core[0]] + first_plane + first_next + first_core[1:]
        + first_last
    ]
    folded_out = kernel(
        fold_out_kernel, [((padded, D), bf)], small, cross_value,
        *first_blocks, scratch=weight_buffer(1),
    )[0]
    mixed, lse, after_cross, hidden, upward, active, after_first, self_in = kernel(
        functools.partial(merge_kernel, channels=channels),
        [
            ((padded, rows), bf), ((1, rows), f32), ((rows, D), f32), ((rows, D), bf),
            ((rows, D), f32), ((rows, D), bf), ((rows, D), f32), ((rows, D), bf),
        ],
        small, received, state, folded_out, gains, *first_blocks,
        scratch=weight_buffer(2),
    )
    self_parts = gather_eight(self_in)
    second_next = from_next(second_plane, self_in)
    second_core = from_core([second_whole] + second_plane, self_in)
    total_rows = positions.shape[1]
    self_rows, head_weights, qkv, self_mixed, self_lse, sent = kernel(
        attend_kernel,
        [
            ((total_rows, D), bf), ((D, 3 * HEAD), bf), ((total_rows, 3 * HEAD), bf),
            ((HEAD, total_rows), f32), ((1, total_rows), f32), ((8, HEAD, BLOCK), bf),
        ],
        small, mine, theirs, limits, places, *self_parts,
    )
    second_last = from_core(second_next, qkv)
    second_blocks = [
        Any(block)
        for block in [second_whole, second_core[0]] + second_plane + second_next
        + second_core[1:] + second_last
    ]
    received = exchange(sent)
    grad_final = swap_half(cotangent[0])
    out, keep, give, quarters, second_gain_part, state_grad, sent = kernel(
        second_kernel,
        [
            ((rows, D), bf), ((4, rows, 512), bf), ((4, rows, 512), bf), ((4, 4, rows, WIDE), bf),
            ((1, D), f32), ((rows, D), f32), ((8, BLOCK, rows), bf),
        ],
        small, received, after_first, grad_final, gains, hidden, active,
        *second_blocks, scratch=weight_buffer(3),
    )
    received = exchange(sent)
    give, early = hold((give, quarters), received)
    gave = swap_row(give)
    early = [early[0], swap_core(early[1]), swap_chip(early[2]), swap_cross(early[3])]
    grad_qkv, sent = kernel(
        attend_back_kernel,
        [((total_rows, 3 * HEAD), bf), ((2, 4, rows, D), bf)],
        small, received, qkv, self_mixed, self_lse, head_weights, limits, places,
    )
    chunk = (2, BLOCK, 6 * HEAD)
    head_keep, head_give = kernel(
        head_weight_kernel, [(chunk, bf), (chunk, bf)], small, self_rows, grad_qkv,
    )
    sent, head_give = hold((sent, head_give), gave, *early[1:])
    head_near = swap_near(head_give)
    summed = low(full(sent[0]) + full(swap_core(sent[1])))
    by_row, by_chip, by_both = swap_row(summed[1]), swap_chip(summed[2]), swap_both(summed[3])
    keep, first_quarter, head_mine, head_next = hold(
        (keep, early[0], plus(head_keep[0], head_near[0]), plus(head_keep[1], head_near[1])),
        by_row, by_chip, by_both,
    )
    kept = swap_chip(keep)
    first_quarter = swap_row(first_quarter)
    head_far = swap_far(head_next)
    gain_rows, last_keep, last_give, last_quarters, cross_grad, value_part, sent = kernel(
        functools.partial(first_back_kernel, channels=channels),
        [
            ((2, D), f32), ((1, rows, 512), bf), ((1, rows, 512), bf), ((4, 1, rows, WIDE), bf),
            ((rows, D), f32), ((padded, D), bf), ((padded, rows), bf),
        ],
        small, summed[0], by_row, by_chip, by_both, state_grad, after_first, after_cross, upward,
        gains, folded_out, mixed, lse, *first_blocks,
        scratch=weight_buffer(2),
    )
    sent, head_far = hold((sent, head_far), kept, first_quarter)
    sent_parts = gather_eight(sent)
    third = hold([gave] + early[1:] + [plus(head_mine, head_far)], *sent_parts[1:])
    gave_chip = swap_chip(third[0])
    other_quarters = [swap_row(part) for part in third[1:4]]
    head_done = third[4]
    head_other = swap_far(head_done)
    grad_rows, input_gain_part, sent = kernel(
        functools.partial(cross_back_kernel, channels=channels),
        [((keys_here, channels), bf), ((1, channels), f32), ((8, padded, BLOCK), bf)],
        small, queries, limits, plain, turned, Any(inputs_here), gain_here, *sent_parts,
        scratch=[
            pltpu.VMEM((8, padded, BLOCK), bf), pltpu.VMEM((keys_here, padded), f32),
            pltpu.VMEM((keys_here, channels), bf), pltpu.SemaphoreType.DMA(()),
        ],
    )
    sent, head_half, gave_chip = hold(
        (sent, jnp.stack([head_done, head_other]), gave_chip), *other_quarters
    )
    received = exchange(sent)
    head_rest = swap_near(head_half)
    early_halves = [keep, gave, kept, gave_chip]
    early_halves = early_halves + from_core(early_halves)
    theirs = [first_quarter] + other_quarters
    early_quarters = [part for k in (0, 2, 1, 3) for part in (early[k], theirs[k])]
    chunk = (2, 3 * BLOCK, WIDE)
    early_keep, early_give = kernel(
        weight_kernel, [(chunk, bf), (chunk, bf)],
        small, *early_halves, *early_quarters,
        scratch=[
            pltpu.VMEM((512, D), bf), pltpu.VMEM((D, WIDE), bf), pltpu.VMEM((2, WIDE, D), bf)
        ],
    )
    received, early_give, last_keep, last_give, last_quarters = hold(
        (received, early_give, last_keep, last_give, last_quarters), head_rest
    )
    early_near = swap_near(early_give)
    last_gave, last_kept = swap_row(last_give), swap_chip(last_keep)
    last_own = [
        last_quarters[0], swap_core(last_quarters[1]), swap_chip(last_quarters[2]),
        swap_cross(last_quarters[3]),
    ]
    wide_part = jnp.pad(input_gain_part, ((0, 0), (0, D - channels)))
    extra = jnp.concatenate([gain_rows, second_gain_part, wide_part], axis=0)
    latents_grad, sent = kernel(
        functools.partial(last_kernel, channels=channels),
        [((rows, D), f32), ((8, 2, padded, BLOCK), bf)],
        received, folded_query, normed_in, state, gains, cross_grad, value_part, extra,
    )
    sent, last_gave, *last_own = hold([sent, last_gave] + last_own, last_kept)
    received_last = exchange(sent)
    last_halves = [last_keep, last_gave, last_kept, swap_chip(last_gave)]
    last_theirs = [swap_row(part) for part in last_own]
    last_parts = [part for k in (0, 2, 1, 3) for part in (last_own[k], last_theirs[k])]
    received_last, *last_halves = hold([received_last] + last_halves, *last_theirs)
    total = kernel(add_kernel, [((2, padded, BLOCK), bf)], received_last)[0]
    last_halves = last_halves + from_core(last_halves, total)
    near = swap_near(total)
    out, latents_grad = hold((out, latents_grad), total)
    chunk = (2, 2 * BLOCK, WIDE)
    last_keep, last_give = kernel(
        last_weight_kernel, [(chunk, bf), (chunk, bf)],
        small, *early_halves, *early_quarters, *last_halves, *last_parts,
        scratch=[pltpu.VMEM((512, D), bf), pltpu.VMEM((D, WIDE), bf), pltpu.VMEM((WIDE, D), bf)],
    )
    head_keep, head_give = kernel(
        head_out_kernel, [((512, 3 * HEAD), bf), ((512, 3 * HEAD), bf)],
        small, head_half, head_rest,
    )
    total, early_mine, early_next, last_give, head_give = hold(
        (
            plus(total, near), plus(early_keep[0], early_near[0]),
            plus(early_keep[1], early_near[1]), last_give, head_give,
        )
    )
    pair = swap_row(head_give)
    far = swap_far(total)
    early_far = swap_far(early_next)
    last_near = swap_near(last_give)
    total, early_done = hold((plus(total, far), plus(early_mine, early_far)), pair)
    total_parts = gather_eight(total)
    early_other = swap_far(early_done)
    early_half, last_mine, last_next, *total_parts = hold(
        [
            jnp.stack([early_done, early_other]), plus(last_keep[0], last_near[0]),
            plus(last_keep[1], last_near[1]),
        ] + total_parts,
    )
    early_rest = swap_near(early_half)
    grad_rows = after(grad_rows, *total_parts[1:])
    last_far = swap_far(last_next)
    grad_cross_query, grad_cross_key, grad_cross_out, grad_cross_value, gain_grads = kernel(
        functools.partial(finish_kernel, channels=channels),
        [
            (cross_query.shape, f32), (cross_key.shape, f32), (cross_out.shape, f32),
            (cross_value.shape, f32), ((5, D), f32),
        ],
        small, cross_key, cross_value, *total_parts,
        *[Any(block) for block in query_blocks], *first_blocks,
        scratch=[pltpu.VMEM((padded, D), bf), pltpu.VMEM((padded, D), bf)]
        + plain_buffer() + weight_buffer(1),
    )
    half = D // 2
    gains_mine = lax.dynamic_slice_in_dim(gain_grads, row * half, half, 1)

    last_done, grad_cross_query = hold((plus(last_mine, last_far), grad_cross_query), early_rest)
    last_other = swap_far(last_done)
    early_sums = kernel(
        weight_out_kernel, [((512, WIDE), f32), ((WIDE, 512), f32), ((WIDE, 512), f32)],
        small, early_half, early_rest,
    )
    last_half = jnp.stack([last_done, last_other])
    last_total = kernel(
        last_weight_out_kernel, [((512, WIDE), f32), ((WIDE, 512), f32)],
        small, last_half, swap_near(last_half),
    )
    keep, pair = full(head_keep), full(pair)
    grad_qkv_weights = [
        in_order(row, keep[:, k * HEAD : (k + 1) * HEAD], pair[:, k * HEAD : (k + 1) * HEAD], 1)
        for k in range(3)
    ]
    other_rows = swap_row(grad_rows)
    return (
        swap_back(out)[None],
        swap_back(latents_grad)[None],
        in_order(row, grad_rows, other_rows, 0)[None],
        gains_mine[0],
        gain_grads[4, :channels],
        grad_cross_query,
        grad_cross_key,
        grad_cross_value,
        grad_cross_out,
        gains_mine[1],
        last_total[0],
        last_total[1],
        gains_mine[2],
        grad_qkv_weights[0],
        grad_qkv_weights[1],
        grad_qkv_weights[2],
        early_sums[2],
        gains_mine[3],
        early_sums[0],
        early_sums[1],
    )


def solution(mesh):
    placed = (
        P("dp", "col", "row"),
        P("dp", "col", None),
        P("dp", None),
        P("dp", None),
        P("dp", "col", "row"),
        P("row"),
        P(),
        P("row", "col"),
        P(),
        P(),
        P("col", "row"),
        P("row"),
        P("row", "col"),
        P("col", "row"),
        P("row"),
        P("row", "col"),
        P("row", "col"),
        P("row", "col"),
        P("col", "row"),
        P("row"),
        P("row", "col"),
        P("col", "row"),
    )
    sizes = dict(mesh.shape)
    quick = sizes == {"row": 2, "col": 4, "dp": 4}
    return jax.shard_map(
        fast_device if quick else on_device,
        mesh=mesh,
        in_specs=placed,
        out_specs=(
            P("dp", "col", "row"),
            P("dp", "col", "row"),
            P("dp", "col", None),
            P("row"),
            P(),
            P("row", "col"),
            P(),
            P(),
            P("col", "row"),
            P("row"),
            P("row", "col"),
            P("col", "row"),
            P("row"),
            P("row", "col"),
            P("row", "col"),
            P("row", "col"),
            P("col", "row"),
            P("row"),
            P("row", "col"),
            P("col", "row"),
        ),
        check_vma=False,
    )
```

```python
import functools
import math

import jax
import jax.numpy as jnp
from jax import lax
from jax.experimental import pallas as pl
from jax.experimental.pallas import tpu as pltpu
from jax.sharding import PartitionSpec as P

D = 1024
HEAD = 128
PIECE_LEN = 256


EPS = 1e-05
NEGATIVE = -1e30
FORWARD_FIRST = "xok,kt->xot"
BACKWARD_FIRST = "tpv,qv->tpq"
FORWARD_SECOND = "ybj,jv->ybv"
BACKWARD_SECOND = "xng,wg->xnw"
GRADIENT_FIRST = "zyq,zyi->qi"
GRADIENT_SECOND = "oqv,oqa->va"


def joined_2(shard, axis, combine):
    everything = jax.tree.map(lambda part: lax.all_gather(part, axis), shard)
    first = jax.tree.map(lambda part: part[0], everything)

    def step(k, so_far):
        return combine(so_far, jax.tree.map(lambda part: part[k], everything))

    return lax.fori_loop(1, lax.axis_size(axis), step, first)


def col_rows(value):
    return lax.all_gather(value, "col", axis=1, tiled=True)


def row_reduce(value):
    return lax.psum_scatter(
        value.astype(jnp.bfloat16), "row", scatter_dimension=1, tiled=True
    ).astype(jnp.float32)


def row_rows(value):
    return lax.all_gather(value, "row", axis=1, tiled=True)


def col_reduce(value):
    return lax.psum_scatter(
        value.astype(jnp.bfloat16), "col", scatter_dimension=1, tiled=True
    ).astype(jnp.float32)


def query_feats(value):
    return lax.all_gather(value, "col", axis=2, tiled=True)


def query_grads(value):
    return lax.psum_scatter(
        value.astype(jnp.bfloat16), "col", scatter_dimension=2, tiled=True
    ).astype(jnp.float32)


def row_totals(first, second):
    return lax.psum((first, second), "row")


def project_cols(value, weight, form):
    gathered = col_rows(value)
    partial_sum = jnp.einsum(form, gathered, weight, preferred_element_type=jnp.float32)
    return (row_reduce(partial_sum), gathered)


def project_rows(value, weight, form):
    gathered = row_rows(value)
    partial_sum = jnp.einsum(form, gathered, weight, preferred_element_type=jnp.float32)
    return (col_reduce(partial_sum), gathered)


def weight_grad(form, first, second):
    return jnp.einsum(form, first, second, preferred_element_type=jnp.float32)


def split_parts(value):
    leading = value.astype(jnp.bfloat16)
    residue = (value - leading.astype(jnp.float32)).astype(jnp.bfloat16)
    return (leading, residue)


def split_einsum(form, exact, other, first_side):
    leading, residue = split_parts(exact)
    if first_side:
        return jnp.einsum(form, leading, other, preferred_element_type=jnp.float32) + jnp.einsum(
            form, residue, other, preferred_element_type=jnp.float32
        )
    return jnp.einsum(form, other, leading, preferred_element_type=jnp.float32) + jnp.einsum(
        form, other, residue, preferred_element_type=jnp.float32
    )


def norm_forward(value, gain):
    width = value.shape[-1] * lax.axis_size("row")
    total, squares = row_totals(jnp.sum(value, axis=-1), jnp.sum(value * value, axis=-1))
    center = total / width
    spread = squares / width - center * center
    scale_inv = lax.rsqrt(spread + EPS)
    normed = (value - center[..., None]) * scale_inv[..., None]
    return (normed * gain, normed, scale_inv)


def norm_backward(grad, gain, normed, scale_inv):
    width = grad.shape[-1] * lax.axis_size("row")
    scaled = grad * gain
    first, second = row_totals(jnp.sum(scaled, axis=-1), jnp.sum(scaled * normed, axis=-1))
    result = scale_inv[..., None] * (
        scaled - first[..., None] / width - normed * (second[..., None] / width)
    )
    return (result, jnp.sum(grad * normed, axis=(0, 1)))


def gelu_exact(value):
    return jax.nn.gelu(value, approximate=False)


def gelu_back(value, grad):
    return jax.vjp(gelu_exact, value)[1](grad)[0]


def view_limits(positions, starts):
    ends = starts + PIECE_LEN
    inside = (starts[:, None, :] <= positions[:, :, None]) & (
        positions[:, :, None] < ends[:, None, :]
    )
    reach = jnp.sum(jnp.where(inside, ends[:, None, :], 0), axis=-1)
    return jnp.maximum(positions + 1, reach)


def merge_softmax(first, second):
    top = jnp.maximum(first[0], second[0])
    return (top, first[1] * jnp.exp(first[0] - top) + second[1] * jnp.exp(second[0] - top))


def feed_forward(state, gain, expand, shrink):
    normed_out, normed, scale_inv = norm_forward(state, gain)
    upward, hidden_rows = project_cols(normed_out.astype(jnp.bfloat16), expand, FORWARD_FIRST)
    activated = gelu_exact(upward).astype(jnp.bfloat16)
    branch, active_rows = project_rows(activated, shrink, FORWARD_SECOND)
    return (state + branch, (normed, scale_inv, hidden_rows, upward, active_rows))


def feed_backward(grad, saved, gain, expand, shrink):
    normed, scale_inv, hidden_rows, upward, active_rows = saved
    grad_active, branch_rows = project_cols(grad.astype(jnp.bfloat16), shrink, BACKWARD_SECOND)
    grad_shrink = weight_grad(GRADIENT_SECOND, active_rows, branch_rows)
    grad_upward = gelu_back(upward, grad_active).astype(jnp.bfloat16)
    grad_hidden, upward_rows = project_rows(grad_upward, expand, BACKWARD_FIRST)
    grad_expand = weight_grad(GRADIENT_FIRST, hidden_rows, upward_rows)
    grad_normed, grad_gain = norm_backward(grad_hidden, gain, normed, scale_inv)
    return (grad + grad_normed, grad_gain, grad_expand, grad_shrink)


def input_back(grad_part, normed, scale_inv, gain):
    scaled = grad_part * gain
    first = jnp.mean(scaled, axis=-1, keepdims=True)
    second = jnp.mean(scaled * normed, axis=-1, keepdims=True)
    return scale_inv[..., None] * (scaled - first - normed * second)


def on_device(
    latents,
    inputs,
    positions,
    piece_start,
    cotangent,
    cross_gain,
    input_gain,
    cross_query,
    cross_key,
    cross_value,
    cross_out,
    first_gain,
    first_expand,
    first_shrink,
    self_gain,
    self_query,
    self_key,
    self_value,
    self_out,
    second_gain,
    second_expand,
    second_shrink,
):
    low_type = jnp.bfloat16
    full_type = jnp.float32
    row_at = lax.axis_index("row")
    col_at = lax.axis_index("col")
    seqs = latents.shape[0]
    total_rows = positions.shape[1]
    rows_here = total_rows // lax.axis_size("row")
    column_width_count = cross_query.shape[1]
    width_row = cross_query.shape[0]
    key_rows = inputs.shape[1]
    heads_here = column_width_count // HEAD
    cross_scale = 1.0 / math.sqrt(D)
    self_scale = 1.0 / math.sqrt(HEAD)
    limit_all = view_limits(positions, piece_start)
    limit_here = lax.dynamic_slice_in_dim(limit_all, row_at * rows_here, rows_here, 1)
    key_index = col_at * key_rows + jnp.arange(key_rows, dtype=jnp.int32)
    cross_mask = key_index[None, None, :] < limit_here[:, :, None]
    latent_attend_mask = (positions[:, None, :] < limit_here[:, :, None])[:, None]
    initial = latents.astype(full_type)
    cross_normed_out, cross_normed, cross_inv = norm_forward(initial, cross_gain)
    query_part, cross_rows = project_cols(
        cross_normed_out.astype(low_type), cross_query, FORWARD_FIRST
    )
    query_all = query_feats(query_part.astype(low_type))
    input_full = inputs.astype(full_type)
    input_center = input_full - jnp.mean(input_full, axis=-1, keepdims=True)
    input_inv = lax.rsqrt(jnp.mean(input_center * input_center, axis=-1) + EPS)
    input_normed = input_center * input_inv[..., None]
    input_low = (input_normed * input_gain).astype(low_type)

    def project_keys(rows):
        key_block = jnp.dot(rows, cross_key, preferred_element_type=full_type).astype(low_type)
        value_block = jnp.dot(rows, cross_value, preferred_element_type=full_type).astype(low_type)
        return (key_block, value_block)

    keys_all, values_all = lax.map(project_keys, input_low)
    scores = (
        jnp.einsum("sqd,skd->sqk", query_all, keys_all, preferred_element_type=full_type)
        * cross_scale
    )
    local_top = jnp.max(jnp.where(cross_mask, scores, NEGATIVE), axis=-1)
    local_total = jnp.sum(
        jnp.where(cross_mask, jnp.exp(scores - local_top[..., None]), 0.0), axis=-1
    )
    merged_top, merged_total = joined_2((local_top, local_total), "col", merge_softmax)
    cross_lse = merged_top + jnp.log(merged_total)
    cross_chances = jnp.where(cross_mask, jnp.exp(scores - cross_lse[..., None]), 0.0).astype(
        low_type
    )
    attended_part = jnp.einsum(
        "sqk,skd->sqd", cross_chances, values_all, preferred_element_type=full_type
    )
    attended_all = lax.psum(attended_part.astype(jnp.bfloat16), "col").astype(jnp.float32)
    attended_here = lax.dynamic_slice_in_dim(
        attended_all, col_at * column_width_count, column_width_count, 2
    )
    cross_branch, attended_rows = project_rows(
        attended_here.astype(low_type), cross_out, FORWARD_SECOND
    )
    after_cross = initial + cross_branch
    after_first, first_saved = feed_forward(after_cross, first_gain, first_expand, first_shrink)
    self_normed_out, self_normed, self_inv = norm_forward(after_first, self_gain)
    joined = jnp.concatenate([self_query, self_key, self_value], axis=1)
    projected, self_rows = project_cols(self_normed_out.astype(low_type), joined, FORWARD_FIRST)
    projected_low = projected.astype(low_type)
    pair_all = row_rows(projected_low[..., column_width_count:])
    heads_q = projected_low[..., :column_width_count].reshape(seqs, rows_here, heads_here, HEAD)
    heads_k = pair_all[..., :column_width_count].reshape(seqs, total_rows, heads_here, HEAD)
    heads_v = pair_all[..., column_width_count:].reshape(seqs, total_rows, heads_here, HEAD)
    self_scores = (
        jnp.einsum("sqhd,skhd->shqk", heads_q, heads_k, preferred_element_type=full_type)
        * self_scale
    )
    self_top = jnp.max(jnp.where(latent_attend_mask, self_scores, NEGATIVE), axis=-1)
    self_total = jnp.sum(
        jnp.where(latent_attend_mask, jnp.exp(self_scores - self_top[..., None]), 0.0), axis=-1
    )
    self_lse = self_top + jnp.log(self_total)
    self_chances = jnp.where(
        latent_attend_mask, jnp.exp(self_scores - self_lse[..., None]), 0.0
    ).astype(low_type)
    self_mixed = jnp.einsum(
        "shqk,skhd->sqhd", self_chances, heads_v, preferred_element_type=full_type
    )
    self_branch, mixed_rows = project_rows(
        self_mixed.reshape(seqs, rows_here, column_width_count).astype(low_type),
        self_out,
        FORWARD_SECOND,
    )
    after_self = after_first + self_branch
    final_state, second_saved = feed_forward(after_self, second_gain, second_expand, second_shrink)
    result = final_state.astype(low_type)
    grad_state = cotangent.astype(full_type)
    grad_state, grad_second_gain, grad_second_expand, grad_second_shrink = feed_backward(
        grad_state, second_saved, second_gain, second_expand, second_shrink
    )
    grad_mixed, self_branch_rows = project_cols(
        grad_state.astype(low_type), self_out, BACKWARD_SECOND
    )
    grad_self_out = weight_grad(GRADIENT_SECOND, mixed_rows, self_branch_rows)
    grad_mixed_low = grad_mixed.astype(low_type).reshape(seqs, rows_here, heads_here, HEAD)
    self_delta = jnp.transpose(
        jnp.sum(grad_mixed_low.astype(full_type) * self_mixed, axis=-1), (0, 2, 1)
    )
    again_scores = (
        jnp.einsum("sqhd,skhd->shqk", heads_q, heads_k, preferred_element_type=full_type)
        * self_scale
    )
    again_chances = jnp.where(latent_attend_mask, jnp.exp(again_scores - self_lse[..., None]), 0.0)
    grad_self_chances = jnp.einsum(
        "sqhd,skhd->shqk", grad_mixed_low, heads_v, preferred_element_type=full_type
    )
    grad_self_scores = (again_chances * (grad_self_chances - self_delta[..., None])).astype(
        low_type
    )
    grad_heads_q = (
        jnp.einsum("shqk,skhd->sqhd", grad_self_scores, heads_k, preferred_element_type=full_type)
        * self_scale
    )
    grad_heads_k = (
        jnp.einsum("shqk,sqhd->skhd", grad_self_scores, heads_q, preferred_element_type=full_type)
        * self_scale
    )
    grad_heads_v = jnp.einsum(
        "shqk,sqhd->skhd",
        again_chances.astype(low_type),
        grad_mixed_low,
        preferred_element_type=full_type,
    )
    pair_grad = row_reduce(
        jnp.concatenate(
            [
                grad_heads_k.reshape(seqs, total_rows, column_width_count),
                grad_heads_v.reshape(seqs, total_rows, column_width_count),
            ],
            axis=-1,
        )
    )
    joined_grad = jnp.concatenate(
        [grad_heads_q.reshape(seqs, rows_here, column_width_count), pair_grad], axis=-1
    ).astype(low_type)
    grad_self_in, joined_rows = project_rows(joined_grad, joined, BACKWARD_FIRST)
    grad_joined = weight_grad(GRADIENT_FIRST, self_rows, joined_rows)
    grad_self_normed, grad_self_gain = norm_backward(grad_self_in, self_gain, self_normed, self_inv)
    grad_state = grad_state + grad_self_normed
    grad_state, grad_first_gain, grad_first_expand, grad_first_shrink = feed_backward(
        grad_state, first_saved, first_gain, first_expand, first_shrink
    )
    grad_attended, cross_branch_rows = project_cols(
        grad_state.astype(low_type), cross_out, BACKWARD_SECOND
    )
    grad_cross_out = weight_grad(GRADIENT_SECOND, attended_rows, cross_branch_rows)
    grad_attended_all = query_feats(grad_attended.astype(low_type))
    cross_delta = jnp.sum(grad_attended_all.astype(full_type) * attended_all, axis=-1)

    def cross_back_one(carry, item):
        query_one, keys_one, values_one, grad_one, lse_one, delta_one, mask_one, normed_one = item
        scores_one = (
            jnp.einsum("qd,kd->qk", query_one, keys_one, preferred_element_type=full_type)
            * cross_scale
        )
        chances_one = jnp.where(mask_one, jnp.exp(scores_one - lse_one[:, None]), 0.0)
        grad_chances = jnp.einsum(
            "qd,kd->qk", grad_one, values_one, preferred_element_type=full_type
        )
        grad_scores = (chances_one * (grad_chances - delta_one[:, None])).astype(low_type)
        grad_query = (
            jnp.einsum("qk,kd->qd", grad_scores, keys_one, preferred_element_type=full_type)
            * cross_scale
        )
        grad_keys = (
            jnp.einsum("qk,qd->kd", grad_scores, query_one, preferred_element_type=full_type)
            * cross_scale
        )
        grad_values = jnp.einsum(
            "qk,qd->kd", chances_one.astype(low_type), grad_one, preferred_element_type=full_type
        )
        grad_normed = split_einsum("kd,cd->kc", grad_keys, cross_key, True) + split_einsum(
            "kd,cd->kc", grad_values, cross_value, True
        )
        key_sum = carry[0] + split_einsum("kc,kd->cd", grad_keys, normed_one, False)
        value_sum = carry[1] + split_einsum("kc,kd->cd", grad_values, normed_one, False)
        return ((key_sum, value_sum), (grad_query, grad_normed))

    empty = jnp.zeros(cross_key.shape, full_type)
    (grad_key_sum, grad_value_sum), (grad_query_all, grad_input_part) = lax.scan(
        cross_back_one,
        (empty, empty),
        (
            query_all,
            keys_all,
            values_all,
            grad_attended_all,
            cross_lse,
            cross_delta,
            cross_mask,
            input_low,
        ),
    )
    grad_query_here = query_grads(grad_query_all).astype(low_type)
    grad_cross_in, query_rows = project_rows(grad_query_here, cross_query, BACKWARD_FIRST)
    grad_cross_query = weight_grad(GRADIENT_FIRST, cross_rows, query_rows)
    grad_cross_normed, grad_cross_gain = norm_backward(
        grad_cross_in, cross_gain, cross_normed, cross_inv
    )
    grad_latents = grad_state + grad_cross_normed
    input_gain_part = jnp.sum(grad_input_part * input_normed, axis=(0, 1))
    summed = lax.psum(grad_input_part.astype(jnp.bfloat16), "row").astype(jnp.float32)
    grad_inputs = input_back(summed, input_normed, input_inv, input_gain).astype(low_type)
    grid = (
        lax.psum(grad_cross_query.astype(jnp.bfloat16), "dp").astype(jnp.float32),
        lax.psum(grad_cross_out.astype(jnp.bfloat16), "dp").astype(jnp.float32),
        lax.psum(grad_first_expand.astype(jnp.bfloat16), "dp").astype(jnp.float32),
        lax.psum(grad_first_shrink.astype(jnp.bfloat16), "dp").astype(jnp.float32),
        lax.psum(grad_joined.astype(jnp.bfloat16), "dp").astype(jnp.float32),
        lax.psum(grad_self_out.astype(jnp.bfloat16), "dp").astype(jnp.float32),
        lax.psum(grad_second_expand.astype(jnp.bfloat16), "dp").astype(jnp.float32),
        lax.psum(grad_second_shrink.astype(jnp.bfloat16), "dp").astype(jnp.float32),
    )
    gains_local = jnp.stack([grad_cross_gain, grad_first_gain, grad_self_gain, grad_second_gain])
    padded = lax.dynamic_update_slice(
        jnp.zeros((4, width_row * lax.axis_size("row")), full_type),
        gains_local,
        (jnp.int32(0), row_at * width_row),
    )
    shared = lax.psum((grad_key_sum, grad_value_sum, padded, input_gain_part), ("row", "col", "dp"))
    gains_all = lax.dynamic_slice_in_dim(shared[2], row_at * width_row, width_row, 1)
    joined_sum = grid[4]
    return (
        result,
        grad_latents,
        grad_inputs,
        gains_all[0],
        shared[3],
        grid[0],
        shared[0],
        shared[1],
        grid[1],
        gains_all[1],
        grid[2],
        grid[3],
        gains_all[2],
        joined_sum[:, :column_width_count],
        joined_sum[:, column_width_count : 2 * column_width_count],
        joined_sum[:, 2 * column_width_count :],
        grid[5],
        gains_all[3],
        grid[6],
        grid[7],
    )


NEG = -1e30
WIDE = 256
BLOCK = 128


def col_step(flip):
    return tuple((c, c ^ flip) for c in range(4))


ROW_SWAP = ((0, 1), (1, 0))
BOTH_SWAP = tuple((r * 4 + c, (1 - r) * 4 + (c ^ 2)) for r in range(2) for c in range(4))
SEQ_NEAR = ((0, 1), (1, 0), (2, 3), (3, 2))
SEQ_FAR = ((0, 2), (2, 0), (1, 3), (3, 1))
GROUP = ("col", "row")


def swap_row(value):
    return lax.ppermute(value, "row", ROW_SWAP)


def swap_chip(value):
    return lax.ppermute(value, "col", col_step(2))


def swap_core(value):
    return lax.ppermute(value, "col", col_step(1))


def swap_both(value):
    return lax.ppermute(value, ("row", "col"), BOTH_SWAP)


def gather_eight(value):
    near = [value, swap_row(value), swap_chip(value), swap_both(value)]
    return near + [swap_core(part) for part in near]


def exchange(value):
    return lax.all_to_all(value, GROUP, 0, 0, tiled=True)


def hold(values, *others):
    return lax.optimization_barrier(tuple(values) + others)[: len(values)]


def after(value, *others):
    return lax.optimization_barrier((value,) + others)[0]


class Any:
    def __init__(self, value):
        self.value = value


class Small:
    def __init__(self, value):
        self.value = value


def kernel(body, outs, *args, scratch=()):
    spaces = {Any: pl.ANY, Small: pltpu.SMEM}
    specs = [pl.BlockSpec(memory_space=spaces.get(type(arg), pltpu.VMEM)) for arg in args]
    values = [arg.value if type(arg) in spaces else arg for arg in args]
    return pl.pallas_call(
        body,
        out_shape=tuple(jax.ShapeDtypeStruct(shape, kind) for shape, kind in outs),
        in_specs=specs,
        out_specs=tuple(pl.BlockSpec(memory_space=pltpu.VMEM) for _ in outs),
        scratch_shapes=list(scratch),
        compiler_params=pltpu.CompilerParams(vmem_limit_bytes=56 * 1024 * 1024),
    )(*values)


def from_plane(half, *others):
    half = after(half, *others)
    return [swap_row(half), swap_chip(half), swap_both(half)]


def from_next(parts, *others):
    parts = lax.optimization_barrier(tuple(parts) + others)[: len(parts)]
    return [lax.ppermute(part, "dp", SEQ_NEAR) for part in parts]


def from_core(parts, *others):
    parts = lax.optimization_barrier(tuple(parts) + others)[: len(parts)]
    return [swap_core(part) for part in parts]


def weight_buffer(count):
    return [pltpu.VMEM((8, 2, count * WIDE, WIDE), jnp.bfloat16), pltpu.SemaphoreType.DMA((16,))]


def load_weights(scalars, blocks, buffer, sems, first):
    height = buffer.shape[2]
    rows = pl.ds(first * WIDE, height)
    plane = scalars[4]
    copies = []
    for core in range(2):
        for half in range(2):
            copies.append((blocks[core].at[half, rows, :], block_of(scalars, 0, core), half))
    for k, block in enumerate(blocks[2:]):
        core, other, step = k // 6, k // 3 % 2, k % 3 + 1
        half = 1 - plane if other else plane
        copies.append((block.at[rows, :], block_of(scalars, step, core), half))
    copies = [
        pltpu.make_async_copy(source, buffer.at[block, half], sems.at[k])
        for k, (source, block, half) in enumerate(copies)
    ]
    for copy in copies:
        copy.start()
    return copies


def load_plain(scalars, blocks, buffer, sems):
    copies = [
        pltpu.make_async_copy(
            block, buffer.at[block_of(scalars, j % 4, j // 4)], sems.at[j]
        )
        for j, block in enumerate(blocks)
    ]
    for copy in copies:
        copy.start()
    return copies


def plain_buffer():
    return [pltpu.VMEM((8, 512, WIDE), jnp.bfloat16), pltpu.SemaphoreType.DMA((8,))]


def wait_all(copies):
    for copy in copies:
        copy.wait()


def mm(a, b):
    return lax.dot_general(a, b, (((1,), (0,)), ((), ())), preferred_element_type=jnp.float32)


def mt(a, b):
    return lax.dot_general(a, b, (((1,), (1,)), ((), ())), preferred_element_type=jnp.float32)


def low(v):
    return v.astype(jnp.bfloat16)


def full(v):
    return v.astype(jnp.float32)


def norm_parts(value):
    width = value.shape[-1]
    center = jnp.sum(value, axis=-1, keepdims=True) / width
    shifted = value - center
    spread = jnp.sum(shifted * shifted, axis=-1, keepdims=True) / width
    inv = lax.rsqrt(spread + EPS)
    return shifted * inv, inv


def norm_back(grad, gain, normed, inv):
    width = grad.shape[-1]
    scaled = grad * gain
    first = jnp.sum(scaled, axis=-1, keepdims=True) / width
    second = jnp.sum(scaled * normed, axis=-1, keepdims=True) / width
    return inv * (scaled - first - normed * second), jnp.sum(grad * normed, axis=0, keepdims=True)


def phi(value):
    return 0.5 * (1.0 + lax.erf(value * (1.0 / math.sqrt(2.0))))


def gelu_value(value):
    return value * phi(value)


def gelu_slope(value):
    return phi(value) + value * jnp.exp(value * value * -0.5) * (1.0 / math.sqrt(2.0 * math.pi))


def three(value):
    first = low(value)
    rest = value - full(first)
    second = low(rest)
    return full(first), full(second), rest - full(second)


def block_of(scalars, step, core):
    return scalars[0] ^ (4 * (step // 2) + 2 * core + step % 2)


def rows_of(count, lanes):
    return lax.broadcasted_iota(jnp.int32, (count, lanes), 0)


def add_kernel(parts, total):
    acc = full(parts[0])
    for b in range(1, parts.shape[0]):
        acc = acc + full(parts[b])
    total[...] = low(acc)


def input_kernel(scalars, inputs, gain, plain, turned, rows, sem):
    count, channels = rows.shape
    at = pl.multiple_of(scalars[1] * count, count)
    copy = pltpu.make_async_copy(inputs.at[pl.ds(at, count), :], rows, sem)
    copy.start()
    plain[...] = jnp.zeros_like(plain)
    turned[...] = jnp.zeros_like(turned)
    copy.wait()
    normed, _ = norm_parts(full(rows[...]))
    result = normed * gain[...]
    plain[:, 0:channels] = low(result)
    turned[0:channels, :] = low(result.T)


def pack_kernel(scalars, query, key, value, *rest):
    weights, (mine, theirs, first, first_half, second, second_half) = rest[:6], rest[7:]
    for k, weight in enumerate((query, key, value)):
        for place, row in ((mine, scalars[1]), (theirs, 1 - scalars[1])):
            at = pl.multiple_of(row * HEAD, HEAD)
            place[:, k * HEAD : (k + 1) * HEAD] = weight[:, pl.ds(at, HEAD)]
    for k, weight in enumerate(weights):
        whole, half = ((first, first_half), (second, second_half))[k // 3]
        rows = slice(k % 3 * WIDE, (k % 3 + 1) * WIDE)
        at = pl.multiple_of(scalars[4] * WIDE, WIDE)
        if weight.shape[0] == WIDE:
            whole[0, rows, :] = weight[:, :WIDE]
            whole[1, rows, :] = weight[:, WIDE:]
            half[rows, :] = weight[:, pl.ds(at, WIDE)]
        else:
            whole[0, rows, :] = weight[:WIDE, :]
            whole[1, rows, :] = weight[WIDE:, :]
            half[rows, :] = weight[pl.ds(at, WIDE), :]


def query_kernel(
    scalars, latents, other, gains, key, *rest
):
    blocks, (state, normed_in, folded, query, wide, buffer, sems) = rest[1:9], rest[9:]
    copies = load_plain(scalars, blocks, buffer, sems)
    row = scalars[1]
    rows = pl.multiple_of(row * BLOCK, BLOCK)
    mine = pl.multiple_of(row * 512, 512)
    theirs = pl.multiple_of((1 - row) * 512, 512)
    state[:, pl.ds(mine, 512)] = latents[pl.ds(rows, BLOCK), :]
    state[:, pl.ds(theirs, 512)] = other[...]
    value, _ = norm_parts(full(state[...]))
    normed_in[...] = low(value * gains[0:1, :])
    channels = key.shape[0]
    folded[...] = jnp.zeros_like(folded)
    wait_all(copies)
    for r in range(2):
        acc = None
        for c in range(4):
            part = mt(key[:, c * WIDE : (c + 1) * WIDE], buffer[2 * c + r])
            acc = part if acc is None else acc + part
        folded[0:channels, r * 512 : (r + 1) * 512] = low(acc)
    query[...] = low(mt(folded[...], normed_in[...]) * (1.0 / math.sqrt(D)))


BULK = 14


def fold_out_kernel(scalars, value, *rest):
    blocks, (folded, buffer, sems) = rest[:BULK], rest[BULK:]
    copies = load_weights(scalars, blocks, buffer, sems, 0)
    channels = value.shape[0]
    folded[...] = jnp.zeros_like(folded)
    wait_all(copies)
    folded[0:channels, :] = low(shrink_tiles(value[...], buffer, 0))


def cross_kernel(scalars, limits, plain, turned, *rest, channels):
    blocks, (queries, result) = rest[:8], rest[8:]
    for j, block in enumerate(blocks):
        queries[block_of(scalars, j % 4, j // 4)] = block[...]
    base = scalars[3]
    count, padded = plain.shape

    def pair(i, carry):
        query = jnp.concatenate([queries[2 * i], queries[2 * i + 1]], axis=1)
        limit = jnp.concatenate([limits[2 * i], limits[2 * i + 1]], axis=1)
        scores = mm(plain[...], query)
        keys = rows_of(count, 2 * BLOCK) + base
        mask = keys < limit
        top = jnp.max(jnp.where(mask, scores, NEG), axis=0, keepdims=True)
        weights = jnp.where(mask, jnp.exp(scores - top), 0.0)
        total = jnp.sum(weights, axis=0, keepdims=True)
        mixed = mm(turned[...], low(weights))
        some = total > 0.0
        mixed = mixed * jnp.where(some, 1.0 / jnp.where(some, total, 1.0), 0.0)
        lse = jnp.where(some, top + jnp.log(jnp.where(some, total, 1.0)), NEG)
        index = rows_of(padded, 2 * BLOCK)
        for k, part in enumerate(three(lse)):
            mixed = jnp.where(index == channels + k, part, mixed)
        mixed = low(mixed)
        result[2 * i] = mixed[:, :BLOCK]
        result[2 * i + 1] = mixed[:, BLOCK:]
        return carry

    lax.fori_loop(0, 4, pair, 0)


def tile_of(packed, c, r, half, at):
    return packed[2 * c + r, half, at * WIDE : (at + 1) * WIDE, :]


def part_of(value, index):
    return value[:, index * WIDE : (index + 1) * WIDE]


def summed(parts):
    acc = parts[0]
    for part in parts[1:]:
        acc = acc + part
    return acc


def expand_tiles(value, packed, at):
    return jnp.concatenate(
        [
            summed(
                [
                    mm(part_of(value, 2 * r + h), tile_of(packed, c, r, h, at))
                    for r in range(2)
                    for h in range(2)
                ]
            )
            for c in range(4)
        ],
        axis=1,
    )


def shrink_tiles(value, packed, at):
    return jnp.concatenate(
        [
            summed([mm(part_of(value, c), tile_of(packed, c, r, h, at)) for c in range(4)])
            for r in range(2)
            for h in range(2)
        ],
        axis=1,
    )


def expand_back(value, packed, at):
    return jnp.concatenate(
        [
            summed([mt(part_of(value, c), tile_of(packed, c, r, h, at)) for c in range(4)])
            for r in range(2)
            for h in range(2)
        ],
        axis=1,
    )


def shrink_back(value, packed, at):
    return jnp.concatenate(
        [
            summed(
                [
                    mt(part_of(value, 2 * r + h), tile_of(packed, c, r, h, at))
                    for r in range(2)
                    for h in range(2)
                ]
            )
            for c in range(4)
        ],
        axis=1,
    )


def merge_kernel(scalars, parts, latents, folded_out, gains, *rest, channels):
    blocks, rest = rest[:BULK], rest[BULK:]
    mixed_out, lse_out, after_cross, hidden, upward, active, after_first, self_in = rest[:8]
    packed, sems = rest[8:]
    copies = load_weights(scalars, blocks, packed, sems, 1)
    lses = []
    for d in range(8):
        rows = full(parts[d, channels : channels + 3, :])
        lses.append(rows[0:1] + rows[1:2] + rows[2:3])
    top = lses[0]
    for item in lses[1:]:
        top = jnp.maximum(top, item)
    total = jnp.zeros_like(top)
    mixed = jnp.zeros(parts.shape[1:], jnp.float32)
    for d in range(8):
        share = jnp.exp(lses[d] - top)
        total = total + share
        mixed = mixed + full(parts[d]) * share
    mixed = low(mixed / total)
    mixed_out[...] = mixed
    lse_out[...] = top + jnp.log(total)
    branch = mm(low(full(mixed).T), folded_out[...])
    state = full(latents[...]) + branch
    after_cross[...] = state
    normed, _ = norm_parts(state)
    hid = low(normed * gains[1:2, :])
    hidden[...] = hid
    wait_all(copies)
    up = expand_tiles(hid, packed, 0)
    upward[...] = up
    act = low(gelu_value(up))
    active[...] = act
    state = state + shrink_tiles(act, packed, 1)
    after_first[...] = state
    normed, _ = norm_parts(state)
    self_in[...] = low(normed * gains[2:3, :])


def attend_kernel(scalars, mine, theirs, limits, places, *rest):
    blocks, (rows_out, weights, qkv_out, mixed_out, lse_out, sent) = rest[:8], rest[8:]
    row = scalars[1]
    weights[pl.ds(pl.multiple_of(row * 512, 512), 512), :] = mine[...]
    weights[pl.ds(pl.multiple_of((1 - row) * 512, 512), 512), :] = theirs[...]
    for j, block in enumerate(blocks):
        at = pl.multiple_of(block_of(scalars, j % 4, j // 4) * BLOCK, BLOCK)
        rows_out[pl.ds(at, BLOCK), :] = block[...]
    qkv_out[...] = low(mm(rows_out[...], weights[...]))
    scale = 1.0 / math.sqrt(HEAD)
    turned = low(full(qkv_out[:, 2 * HEAD :]).T)

    def pair(i, carry):
        at = pl.multiple_of(i * WIDE, WIDE)
        query = qkv_out[pl.ds(at, WIDE), 0:HEAD]
        scores = mt(qkv_out[:, HEAD : 2 * HEAD], query) * scale
        limit = jnp.concatenate([limits[2 * i], limits[2 * i + 1]], axis=1)
        mask = places[...] < limit
        top = jnp.max(jnp.where(mask, scores, NEG), axis=0, keepdims=True)
        share = jnp.where(mask, jnp.exp(scores - top), 0.0)
        total = jnp.sum(share, axis=0, keepdims=True)
        mixed = mm(turned, low(share)) / total
        mixed_out[:, pl.ds(at, WIDE)] = mixed
        lse_out[:, pl.ds(at, WIDE)] = top + jnp.log(total)
        lower = low(mixed)
        sent[2 * i] = lower[:, :BLOCK]
        sent[2 * i + 1] = lower[:, BLOCK:]
        return carry

    lax.fori_loop(0, 4, pair, 0)


def split_halves(scalars, values, keep, give):
    row = scalars[1]
    for k, value in enumerate(values):
        low_half, high_half = value[:, :512], value[:, 512:]
        keep[k] = jnp.where(row == 0, low_half, high_half)
        give[k] = jnp.where(row == 0, high_half, low_half)


def split_quarters(scalars, values, quarters):
    for k, value in enumerate(values):
        for c in range(4):
            quarters[scalars[2] ^ c, k] = part_of(value, c)


def second_kernel(scalars, parts, after_first, cotangent, gains, early_hidden, early_active, *rest):
    blocks, rest = rest[:BULK], rest[BULK:]
    out, keep, give, quarters, grad_gain, state_grad, sent = rest[:7]
    packed, sems = rest[7:]
    gain = gains[3:4, :]
    copies = load_weights(scalars, blocks, packed, sems, 0)
    att = low(jnp.concatenate([full(parts[h]).T for h in range(8)], axis=1))
    wait_all(copies)
    state = after_first[...] + shrink_tiles(att, packed, 0)
    normed, inv = norm_parts(state)
    hid = low(normed * gain)
    up = expand_tiles(hid, packed, 1)
    act = low(gelu_value(up))
    out[...] = low(state + shrink_tiles(act, packed, 2))
    grad = cotangent[...]
    gu = low(shrink_back(grad, packed, 2) * gelu_slope(up))
    back, grad_gain[...] = norm_back(expand_back(gu, packed, 1), gain, normed, inv)
    total = full(grad) + back
    state_grad[...] = total
    lower = low(total)
    grad_att = shrink_back(lower, packed, 0)
    for h in range(8):
        sent[h] = low(grad_att[:, h * BLOCK : (h + 1) * BLOCK].T)
    split_halves(scalars, (hid, grad, lower, early_hidden[...]), keep, give)
    split_quarters(scalars, (gu, act, att, early_active[...]), quarters)


def put_chunk(scalars, keep, give, index, value):
    here = scalars[4] == index // 2
    at = scalars[5] ^ (index % 2)

    @pl.when(here)
    def _():
        keep[at] = value

    @pl.when(jnp.logical_not(here))
    def _():
        give[at] = value


def read_chunk(scalars, mine, theirs, index):
    at = scalars[5] ^ (index % 2)
    return jnp.where(scalars[4] == index // 2, full(mine[at]), full(theirs[at]))


def columns(value, index):
    return value[:, index * BLOCK : (index + 1) * BLOCK]


def row_block(value, index):
    return value[index * BLOCK : (index + 1) * BLOCK, :]


def weight_kernel(scalars, *refs):
    halves, quarters, rest = refs[:8], refs[8:16], refs[16:]
    keep, give, halves_turned, quarters_all, quarters_turned = rest
    for k in range(3):
        for j in range(8):
            at = slice(j * BLOCK, (j + 1) * BLOCK)
            if k == 0:
                halves_turned[:, at] = low(full(halves[j][k]).T)
                quarters_all[at, :] = quarters[j][k]
            else:
                quarters_turned[k - 1, :, at] = low(full(quarters[j][k]).T)
    expand = low(mm(halves_turned[...], quarters_all[...]))
    shrinks = [
        low(summed([
            mm(quarters_turned[k - 1, :, j * BLOCK : (j + 1) * BLOCK], halves[j][k])
            for j in range(8)
        ]))
        for k in (1, 2)
    ]
    for t in range(4):
        parts = jnp.concatenate([columns(value, t) for value in shrinks], axis=1)
        put_chunk(scalars, keep, give, t, jnp.concatenate([row_block(expand, t), parts], axis=0))


def weight_out_kernel(scalars, mine, theirs, expand, first_shrink, second_shrink):
    for t in range(4):
        chunk = read_chunk(scalars, mine, theirs, t)
        at = slice(t * BLOCK, (t + 1) * BLOCK)
        expand[at, :] = chunk[:BLOCK]
        first_shrink[:, at] = chunk[BLOCK:, :BLOCK]
        second_shrink[:, at] = chunk[BLOCK:, BLOCK:]


def last_weight_kernel(scalars, *refs):
    early_halves, early_quarters, halves, quarters = refs[:8], refs[8:16], refs[16:24], refs[24:32]
    keep, give, halves_turned, quarters_all, quarters_turned = refs[32:]
    for j in range(8):
        at = slice(j * BLOCK, (j + 1) * BLOCK)
        halves_turned[:, at] = low(full(early_halves[j][3]).T)
        quarters_all[at, :] = quarters[j][0]
        quarters_turned[:, at] = low(full(early_quarters[j][3]).T)
    expand = low(mm(halves_turned[...], quarters_all[...]))
    shrink = low(summed([
        mm(quarters_turned[:, j * BLOCK : (j + 1) * BLOCK], halves[j][0]) for j in range(8)
    ]))
    for t in range(4):
        part = columns(shrink, t)
        parts = jnp.concatenate([part[:BLOCK], part[BLOCK:]], axis=1)
        put_chunk(scalars, keep, give, t, jnp.concatenate([row_block(expand, t), parts], axis=0))


def last_weight_out_kernel(scalars, mine, theirs, expand, shrink):
    for t in range(4):
        chunk = read_chunk(scalars, mine, theirs, t)
        at = slice(t * BLOCK, (t + 1) * BLOCK)
        expand[at, :] = chunk[:BLOCK]
        shrink[:BLOCK, at] = chunk[BLOCK:, :BLOCK]
        shrink[BLOCK:, at] = chunk[BLOCK:, BLOCK:]


def head_weight_kernel(scalars, rows, grads, keep, give):
    turned = low(full(grads[...]).T)
    total = mm(turned, rows[...]).T
    row = scalars[1]
    mine = low(jnp.where(row == 0, total[:512], total[512:]))
    theirs = low(jnp.where(row == 0, total[512:], total[:512]))
    for t in range(4):
        put_chunk(
            scalars, keep, give, t,
            jnp.concatenate([row_block(mine, t), row_block(theirs, t)], axis=1),
        )


def head_out_kernel(scalars, mine, theirs, keep, give):
    width = keep.shape[1]
    for t in range(4):
        chunk = low(read_chunk(scalars, mine, theirs, t))
        at = slice(t * BLOCK, (t + 1) * BLOCK)
        keep[at, :] = chunk[:, :width]
        give[at, :] = chunk[:, width:]


def attend_back_kernel(
    scalars, parts, qkv, mixed, lse, weights, limits, places, grads, sent
):
    scale = 1.0 / math.sqrt(HEAD)
    keys_turned = low(full(qkv[:, HEAD : 2 * HEAD]).T)

    def pair(i, carry):
        grad_k, grad_v = carry
        at = pl.multiple_of(i * WIDE, WIDE)
        query = qkv[pl.ds(at, WIDE), 0:HEAD]
        grad_out = jnp.concatenate([parts[2 * i], parts[2 * i + 1]], axis=1)
        delta = jnp.sum(full(grad_out) * mixed[:, pl.ds(at, WIDE)], axis=0, keepdims=True)
        scores = mt(qkv[:, HEAD : 2 * HEAD], query) * scale
        limit = jnp.concatenate([limits[2 * i], limits[2 * i + 1]], axis=1)
        mask = places[...] < limit
        share = jnp.where(mask, jnp.exp(scores - lse[:, pl.ds(at, WIDE)]), 0.0)
        grad_share = mm(qkv[:, 2 * HEAD :], grad_out)
        grad_scores = low(share * (grad_share - delta))
        grad_k = grad_k + mm(grad_scores, query)
        grad_v = grad_v + mt(low(share), grad_out)
        grad_q = mm(keys_turned, grad_scores) * scale
        grads[pl.ds(at, WIDE), 0:HEAD] = low(grad_q.T)
        return grad_k, grad_v

    zero = jnp.zeros((qkv.shape[0], HEAD), jnp.float32)
    grad_k, grad_v = lax.fori_loop(0, 4, pair, (zero, zero))
    grads[:, HEAD : 2 * HEAD] = low(grad_k * scale)
    grads[:, 2 * HEAD :] = low(grad_v)
    for step in range(4):
        for core in range(2):
            at = pl.multiple_of(block_of(scalars, step, core) * BLOCK, BLOCK)
            sent[core, step] = low(mt(grads[pl.ds(at, BLOCK), :], weights[...]))


def first_back_kernel(
    scalars, own, by_row, by_chip, by_both, state_grad, after_first, after_cross, upward, gains,
    folded_out, mixed, lse, *rest, channels
):
    blocks, rest = rest[:BULK], rest[BULK:]
    gain_grads, keep, give, quarters, cross_grad, value_part, sent = rest[:7]
    packed, sems = rest[7:]
    copies = load_weights(scalars, blocks, packed, sems, 1)
    grad_in = full(own[...]) + full(by_row[...]) + full(by_chip[...]) + full(by_both[...])
    normed, inv = norm_parts(after_first[...])
    back, self_gain = norm_back(grad_in, gains[2:3, :], normed, inv)
    grad = state_grad[...] + back
    lower = low(grad)
    wait_all(copies)
    gu = low(shrink_back(lower, packed, 1) * gelu_slope(upward[...]))
    split_halves(scalars, (lower,), keep, give)
    split_quarters(scalars, (gu,), quarters)
    grad_hid = expand_back(gu, packed, 0)
    normed, inv = norm_parts(after_cross[...])
    back, first_gain = norm_back(grad_hid, gains[1:2, :], normed, inv)
    gain_grads[0:1, :] = first_gain
    gain_grads[1:2, :] = self_gain
    grad = grad + back
    cross_grad[...] = grad
    lower = low(grad)
    value_part[...] = low(mm(mixed[...], lower))
    grad_mixed = mt(folded_out[...], lower)
    padded = grad_mixed.shape[0]
    index = rows_of(padded, BLOCK)
    grad_mixed = jnp.where(index < channels, grad_mixed, 0.0)
    rounded = full(low(grad_mixed))
    delta = jnp.sum(rounded * full(mixed[...]), axis=0, keepdims=True)
    for k, part in enumerate(three(lse[...]) + three(delta)):
        grad_mixed = jnp.where(index == channels + k, part, grad_mixed)
    sent[...] = low(grad_mixed)


def cross_back_kernel(scalars, queries, limits, plain, turned, inputs, gain, *rest, channels):
    blocks, (grad_rows, grad_gain, sent, grads, total, rows, sem) = rest[:8], rest[8:]
    at = pl.multiple_of(scalars[1] * rows.shape[0], rows.shape[0])
    copy = pltpu.make_async_copy(inputs.at[pl.ds(at, rows.shape[0]), :], rows, sem)
    copy.start()
    for j, block in enumerate(blocks):
        grads[block_of(scalars, j % 4, j // 4)] = block[...]
    base = scalars[3]
    count, padded = plain.shape
    total[...] = jnp.zeros_like(total)

    def pair(i, carry):
        query = jnp.concatenate([queries[2 * i], queries[2 * i + 1]], axis=1)
        grad_mixed = jnp.concatenate([grads[2 * i], grads[2 * i + 1]], axis=1)
        extra = full(grad_mixed[channels : channels + 6, :])
        lse = extra[0:1] + extra[1:2] + extra[2:3]
        delta = extra[3:4] + extra[4:5] + extra[5:6]
        limit = jnp.concatenate([limits[2 * i], limits[2 * i + 1]], axis=1)
        mask = rows_of(count, 2 * BLOCK) + base < limit
        scores = mm(plain[...], query)
        share = jnp.where(mask, jnp.exp(scores - lse), 0.0)
        grad_share = mm(plain[...], grad_mixed)
        grad_scores = low(share * (grad_share - delta))
        out = low(mm(turned[...], grad_scores) * (1.0 / math.sqrt(D)))
        sent[2 * i] = out[:, :BLOCK]
        sent[2 * i + 1] = out[:, BLOCK:]
        total[...] += mt(grad_scores, query) + mt(low(share), grad_mixed)
        return carry

    lax.fori_loop(0, 4, pair, 0)
    copy.wait()
    normed, inv = norm_parts(full(rows[...]))
    back, wide = norm_back(total[:, 0:channels], gain[...], normed, inv)
    grad_gain[...] = wide
    grad_rows[...] = low(back)


def last_kernel(
    parts, folded_query, normed_in, latents, gains, cross_grad, value_part, gain_rows,
    grad_latents, sent, *, channels
):
    acc = full(parts[0])
    for d in range(1, 8):
        acc = acc + full(parts[d])
    padded = acc.shape[0]
    index = rows_of(padded, BLOCK)
    acc = jnp.where(index < channels, acc, 0.0)
    grad_query = low(acc)
    grad_in = mm(low(acc.T), folded_query[...])
    normed, inv = norm_parts(full(latents[...]))
    back, cross_gain = norm_back(grad_in, gains[0:1, :], normed, inv)
    grad_latents[...] = cross_grad[...] + back
    part = mm(grad_query, normed_in[...])
    wide = rows_of(padded, part.shape[1])
    rows = [cross_gain] + [gain_rows[k : k + 1, :] for k in range(4)]
    for k, row in enumerate(rows):
        high = low(row)
        part = jnp.where(wide == channels + 2 * k, full(high), part)
        part = jnp.where(wide == channels + 2 * k + 1, row - full(high), part)
    part = low(part)
    for b in range(8):
        sent[b, 0] = part[:, b * BLOCK : (b + 1) * BLOCK]
        sent[b, 1] = value_part[:, b * BLOCK : (b + 1) * BLOCK]


def finish_kernel(scalars, key, value, *rest, channels):
    blocks, query_blocks, rest = rest[:8], rest[8:16], rest[16:]
    out_blocks, rest = rest[:BULK], rest[BULK:]
    grad_query, grad_key, grad_out, grad_value, gain_grads = rest[:5]
    key_sum, value_sum, packed, sems, packed_out, out_sems = rest[5:]
    copies = load_plain(scalars, query_blocks, packed, sems)
    copies += load_weights(scalars, out_blocks, packed_out, out_sems, 0)
    for j, block in enumerate(blocks):
        at = pl.multiple_of(block_of(scalars, j % 4, j // 4) * BLOCK, BLOCK)
        key_sum[:, pl.ds(at, BLOCK)] = block[0]
        value_sum[:, pl.ds(at, BLOCK)] = block[1]
    extra = full(key_sum[channels : channels + 10, :])
    for k in range(5):
        gain_grads[k : k + 1, :] = extra[2 * k : 2 * k + 1] + extra[2 * k + 1 : 2 * k + 2]
    at = pl.multiple_of(scalars[2] * WIDE, WIDE)
    half = pl.multiple_of(scalars[1] * 512, 512)
    turned = full(key_sum[:, pl.ds(half, 512)]).T
    grad_query[...] = mm(low(turned[:, :channels]), key[:, pl.ds(at, WIDE)])
    turned = full(value[:, pl.ds(at, WIDE)]).T
    grad_out[...] = mm(low(turned), value_sum[0:channels, pl.ds(half, 512)])
    wait_all(copies)
    for c in range(4):
        acc = mm(key_sum[:, 0:512], packed[2 * c]) + mm(key_sum[:, 512:1024], packed[2 * c + 1])
        grad_key[:, c * WIDE : (c + 1) * WIDE] = acc[:channels]
    grad_value[...] = shrink_back(value_sum[...], packed_out, 0)[:channels]


def wide_rows(value, row):
    half = value.shape[1] // 2
    keep = lax.dynamic_slice_in_dim(value, row * half, half, 1)
    give = lax.dynamic_slice_in_dim(value, (1 - row) * half, half, 1)
    return keep, give


def swap_near(value):
    return lax.ppermute(value, "dp", SEQ_NEAR)


def swap_far(value):
    return lax.ppermute(value, "dp", SEQ_FAR)


def plus(a, b):
    return low(full(a) + full(b))


def swap_cross(value):
    return lax.ppermute(value, "col", col_step(3))


def spread_halves(keep, give):
    mine = [keep, swap_row(give)]
    mine = mine + [swap_chip(part) for part in mine]
    return mine + [swap_core(part) for part in mine]


def spread_quarters(quarters):
    mine = [quarters[0], swap_chip(quarters[2]), swap_core(quarters[1]), swap_cross(quarters[3])]
    theirs = [swap_row(part) for part in mine]
    return [mine[0], theirs[0], mine[1], theirs[1], mine[2], theirs[2], mine[3], theirs[3]]


def over_planes(parts):
    count = parts.shape[0] // 4
    at = lax.axis_index("dp")
    pieces = parts.reshape(4, count, parts.shape[1])
    total = low(jnp.sum(full(lax.all_to_all(pieces, "dp", 0, 0, tiled=True)), axis=0))
    return lax.all_gather(total, "dp", axis=0, tiled=True)


def in_order(row, own, other, axis):
    return jnp.where(
        row == 0,
        jnp.concatenate([own, other], axis),
        jnp.concatenate([other, own], axis),
    )


def tiles_of(weight):
    return [weight[:, :WIDE], weight[:, WIDE:]]


def fast_device(
    latents, inputs, positions, piece_start, cotangent, cross_gain, input_gain, cross_query,
    cross_key, cross_value, cross_out, first_gain, first_expand, first_shrink, self_gain,
    self_query, self_key, self_value, self_out, second_gain, second_expand, second_shrink,
):
    bf, f32 = jnp.bfloat16, jnp.float32
    row, col = lax.axis_index("row"), lax.axis_index("col")
    chip, core = col // 2, col % 2
    channels = inputs.shape[-1]
    padded = -(-(channels + 11) // 16) * 16
    keys_here = inputs.shape[1] // 2
    base = col * inputs.shape[1] + row * keys_here
    plane = lax.axis_index("dp") % 2
    far_plane = lax.axis_index("dp") // 2
    scalars = jnp.stack([2 * col + row, row, col, base, plane, far_plane]).astype(jnp.int32)
    rows = BLOCK

    def swap_half(block):
        keep = lax.dynamic_slice_in_dim(block, row * rows, rows, 0)
        give = lax.dynamic_slice_in_dim(block, (1 - row) * rows, rows, 0)
        return in_order(row, keep, swap_row(give), 1)

    def swap_back(value):
        keep, give = wide_rows(value, row)
        return in_order(row, keep, swap_row(give), 0)

    small = Small(scalars)
    inputs_here = inputs[0]
    gain_here = input_gain[None]
    gains_here = jnp.stack([cross_gain, first_gain, self_gain, second_gain])
    other_rows = swap_row(
        lax.dynamic_slice_in_dim(latents[0], (1 - row) * rows, rows, 0)
    )
    query_blocks = [cross_query] + from_plane(cross_query)
    gains = in_order(row, gains_here, swap_row(gains_here), 1)
    plain, turned = kernel(
        input_kernel,
        [((keys_here, padded), bf), ((padded, keys_here), bf)],
        small, Any(inputs_here), gain_here,
        scratch=[pltpu.VMEM((keys_here, channels), bf), pltpu.SemaphoreType.DMA(())],
    )
    whole, half = (2, 3 * WIDE, WIDE), (3 * WIDE, WIDE)
    mine, theirs, first_whole, first_half, second_whole, second_half = kernel(
        pack_kernel,
        [((512, 3 * HEAD), bf), ((512, 3 * HEAD), bf), (whole, bf), (half, bf), (whole, bf),
         (half, bf)],
        small, self_query, self_key, self_value, cross_out, first_expand, first_shrink, self_out,
        second_expand, second_shrink, Any(plain),
    )
    first_plane = from_plane(first_half, other_rows, gains)
    limits = view_limits(positions, piece_start)[0].reshape(8, 1, BLOCK)
    places = positions[0][:, None]
    query_blocks = query_blocks + from_core(query_blocks, plain)
    state, normed_in, folded_query, query = kernel(
        query_kernel,
        [((rows, D), bf), ((rows, D), bf), ((padded, D), bf), ((padded, rows), bf)],
        small, latents[0], other_rows, gains, cross_key, Any(plain),
        *[Any(block) for block in query_blocks],
        scratch=[pltpu.VMEM((8, BLOCK), f32)] + plain_buffer(),
    )
    query_parts = gather_eight(query)
    theirs = swap_row(after(theirs, query))
    first_next = from_next(first_plane, query)
    queries, partial_mixed = kernel(
        functools.partial(cross_kernel, channels=channels),
        [((8, padded, BLOCK), bf), ((8, padded, BLOCK), bf)],
        small, limits, plain, turned, *query_parts,
    )
    received = exchange(partial_mixed)
    first_core = from_core([first_whole] + first_plane, partial_mixed)
    second_plane = from_plane(second_half, received)
    first_last = from_core(first_next, received)
    first_blocks = [
        Any(block)
        for block in [first_whole, first_core[0]] + first_plane + first_next + first_core[1:]
        + first_last
    ]
    folded_out = kernel(
        fold_out_kernel, [((padded, D), bf)], small, cross_value,
        *first_blocks, scratch=weight_buffer(1),
    )[0]
    mixed, lse, after_cross, hidden, upward, active, after_first, self_in = kernel(
        functools.partial(merge_kernel, channels=channels),
        [
            ((padded, rows), bf), ((1, rows), f32), ((rows, D), f32), ((rows, D), bf),
            ((rows, D), f32), ((rows, D), bf), ((rows, D), f32), ((rows, D), bf),
        ],
        small, received, state, folded_out, gains, *first_blocks,
        scratch=weight_buffer(2),
    )
    self_parts = gather_eight(self_in)
    second_next = from_next(second_plane, self_in)
    second_core = from_core([second_whole] + second_plane, self_in)
    total_rows = positions.shape[1]
    self_rows, head_weights, qkv, self_mixed, self_lse, sent = kernel(
        attend_kernel,
        [
            ((total_rows, D), bf), ((D, 3 * HEAD), bf), ((total_rows, 3 * HEAD), bf),
            ((HEAD, total_rows), f32), ((1, total_rows), f32), ((8, HEAD, BLOCK), bf),
        ],
        small, mine, theirs, limits, places, *self_parts,
    )
    second_last = from_core(second_next, qkv)
    second_blocks = [
        Any(block)
        for block in [second_whole, second_core[0]] + second_plane + second_next
        + second_core[1:] + second_last
    ]
    received = exchange(sent)
    grad_final = swap_half(cotangent[0])
    out, keep, give, quarters, second_gain_part, state_grad, sent = kernel(
        second_kernel,
        [
            ((rows, D), bf), ((4, rows, 512), bf), ((4, rows, 512), bf), ((4, 4, rows, WIDE), bf),
            ((1, D), f32), ((rows, D), f32), ((8, BLOCK, rows), bf),
        ],
        small, received, after_first, grad_final, gains, hidden, active,
        *second_blocks, scratch=weight_buffer(3),
    )
    received = exchange(sent)
    give, early = hold((give, quarters), received)
    gave = swap_row(give)
    early = [early[0], swap_core(early[1]), swap_chip(early[2]), swap_cross(early[3])]
    grad_qkv, sent = kernel(
        attend_back_kernel,
        [((total_rows, 3 * HEAD), bf), ((2, 4, rows, D), bf)],
        small, received, qkv, self_mixed, self_lse, head_weights, limits, places,
    )
    chunk = (2, BLOCK, 6 * HEAD)
    head_keep, head_give = kernel(
        head_weight_kernel, [(chunk, bf), (chunk, bf)], small, self_rows, grad_qkv,
    )
    sent, head_give = hold((sent, head_give), gave, *early[1:])
    head_near = swap_near(head_give)
    summed = low(full(sent[0]) + full(swap_core(sent[1])))
    by_row, by_chip, by_both = swap_row(summed[1]), swap_chip(summed[2]), swap_both(summed[3])
    keep, first_quarter, head_mine, head_next = hold(
        (keep, early[0], plus(head_keep[0], head_near[0]), plus(head_keep[1], head_near[1])),
        by_row, by_chip, by_both,
    )
    kept = swap_chip(keep)
    first_quarter = swap_row(first_quarter)
    head_far = swap_far(head_next)
    gain_rows, last_keep, last_give, last_quarters, cross_grad, value_part, sent = kernel(
        functools.partial(first_back_kernel, channels=channels),
        [
            ((2, D), f32), ((1, rows, 512), bf), ((1, rows, 512), bf), ((4, 1, rows, WIDE), bf),
            ((rows, D), f32), ((padded, D), bf), ((padded, rows), bf),
        ],
        small, summed[0], by_row, by_chip, by_both, state_grad, after_first, after_cross, upward,
        gains, folded_out, mixed, lse, *first_blocks,
        scratch=weight_buffer(2),
    )
    sent, head_far = hold((sent, head_far), kept, first_quarter)
    sent_parts = gather_eight(sent)
    third = hold([gave] + early[1:] + [plus(head_mine, head_far)], *sent_parts[1:])
    gave_chip = swap_chip(third[0])
    other_quarters = [swap_row(part) for part in third[1:4]]
    head_done = third[4]
    head_other = swap_far(head_done)
    grad_rows, input_gain_part, sent = kernel(
        functools.partial(cross_back_kernel, channels=channels),
        [((keys_here, channels), bf), ((1, channels), f32), ((8, padded, BLOCK), bf)],
        small, queries, limits, plain, turned, Any(inputs_here), gain_here, *sent_parts,
        scratch=[
            pltpu.VMEM((8, padded, BLOCK), bf), pltpu.VMEM((keys_here, padded), f32),
            pltpu.VMEM((keys_here, channels), bf), pltpu.SemaphoreType.DMA(()),
        ],
    )
    sent, head_half, gave_chip = hold(
        (sent, jnp.stack([head_done, head_other]), gave_chip), *other_quarters
    )
    received = exchange(sent)
    head_rest = swap_near(head_half)
    early_halves = [keep, gave, kept, gave_chip]
    early_halves = early_halves + from_core(early_halves)
    theirs = [first_quarter] + other_quarters
    early_quarters = [part for k in (0, 2, 1, 3) for part in (early[k], theirs[k])]
    chunk = (2, 3 * BLOCK, WIDE)
    early_keep, early_give = kernel(
        weight_kernel, [(chunk, bf), (chunk, bf)],
        small, *early_halves, *early_quarters,
        scratch=[
            pltpu.VMEM((512, D), bf), pltpu.VMEM((D, WIDE), bf), pltpu.VMEM((2, WIDE, D), bf)
        ],
    )
    received, early_give, last_keep, last_give, last_quarters = hold(
        (received, early_give, last_keep, last_give, last_quarters), head_rest
    )
    early_near = swap_near(early_give)
    last_gave, last_kept = swap_row(last_give), swap_chip(last_keep)
    last_own = [
        last_quarters[0], swap_core(last_quarters[1]), swap_chip(last_quarters[2]),
        swap_cross(last_quarters[3]),
    ]
    wide_part = jnp.pad(input_gain_part, ((0, 0), (0, D - channels)))
    extra = jnp.concatenate([gain_rows, second_gain_part, wide_part], axis=0)
    latents_grad, sent = kernel(
        functools.partial(last_kernel, channels=channels),
        [((rows, D), f32), ((8, 2, padded, BLOCK), bf)],
        received, folded_query, normed_in, state, gains, cross_grad, value_part, extra,
    )
    sent, last_gave, *last_own = hold([sent, last_gave] + last_own, last_kept)
    received_last = exchange(sent)
    last_halves = [last_keep, last_gave, last_kept, swap_chip(last_gave)]
    last_theirs = [swap_row(part) for part in last_own]
    last_parts = [part for k in (0, 2, 1, 3) for part in (last_own[k], last_theirs[k])]
    received_last, *last_halves = hold([received_last] + last_halves, *last_theirs)
    total = kernel(add_kernel, [((2, padded, BLOCK), bf)], received_last)[0]
    last_halves = last_halves + from_core(last_halves, total)
    near = swap_near(total)
    out, latents_grad = hold((out, latents_grad), total)
    chunk = (2, 2 * BLOCK, WIDE)
    last_keep, last_give = kernel(
        last_weight_kernel, [(chunk, bf), (chunk, bf)],
        small, *early_halves, *early_quarters, *last_halves, *last_parts,
        scratch=[pltpu.VMEM((512, D), bf), pltpu.VMEM((D, WIDE), bf), pltpu.VMEM((WIDE, D), bf)],
    )
    head_keep, head_give = kernel(
        head_out_kernel, [((512, 3 * HEAD), bf), ((512, 3 * HEAD), bf)],
        small, head_half, head_rest,
    )
    total, early_mine, early_next, last_give, head_give = hold(
        (
            plus(total, near), plus(early_keep[0], early_near[0]),
            plus(early_keep[1], early_near[1]), last_give, head_give,
        )
    )
    pair = swap_row(head_give)
    far = swap_far(total)
    early_far = swap_far(early_next)
    last_near = swap_near(last_give)
    total, early_done, last_next = hold(
        (
            plus(total, far), plus(early_mine, early_far), plus(last_keep[1], last_near[1]),
        ),
        pair,
    )
    total_parts = gather_eight(total)
    early_other = swap_far(early_done)
    last_far = swap_far(last_next)
    early_half, last_done, *total_parts = hold(
        [
            jnp.stack([early_done, early_other]),
            plus(plus(last_keep[0], last_near[0]), last_far),
        ] + total_parts,
    )
    early_rest = swap_near(early_half)
    last_other = swap_far(last_done)
    grad_rows = after(grad_rows, *total_parts[1:])
    last_far = swap_far(last_next)
    grad_cross_query, grad_cross_key, grad_cross_out, grad_cross_value, gain_grads = kernel(
        functools.partial(finish_kernel, channels=channels),
        [
            (cross_query.shape, f32), (cross_key.shape, f32), (cross_out.shape, f32),
            (cross_value.shape, f32), ((5, D), f32),
        ],
        small, cross_key, cross_value, *total_parts,
        *[Any(block) for block in query_blocks], *first_blocks,
        scratch=[pltpu.VMEM((padded, D), bf), pltpu.VMEM((padded, D), bf)]
        + plain_buffer() + weight_buffer(1),
    )
    half = D // 2
    gains_mine = lax.dynamic_slice_in_dim(gain_grads, row * half, half, 1)

    early_sums = kernel(
        weight_out_kernel, [((512, WIDE), f32), ((WIDE, 512), f32), ((WIDE, 512), f32)],
        small, early_half, early_rest,
    )
    last_half = jnp.stack([last_done, last_other])
    last_total = kernel(
        last_weight_out_kernel, [((512, WIDE), f32), ((WIDE, 512), f32)],
        small, last_half, swap_near(last_half),
    )
    keep, pair = full(head_keep), full(pair)
    grad_qkv_weights = [
        in_order(row, keep[:, k * HEAD : (k + 1) * HEAD], pair[:, k * HEAD : (k + 1) * HEAD], 1)
        for k in range(3)
    ]
    other_rows = swap_row(grad_rows)
    return (
        swap_back(out)[None],
        swap_back(latents_grad)[None],
        in_order(row, grad_rows, other_rows, 0)[None],
        gains_mine[0],
        gain_grads[4, :channels],
        grad_cross_query,
        grad_cross_key,
        grad_cross_value,
        grad_cross_out,
        gains_mine[1],
        last_total[0],
        last_total[1],
        gains_mine[2],
        grad_qkv_weights[0],
        grad_qkv_weights[1],
        grad_qkv_weights[2],
        early_sums[2],
        gains_mine[3],
        early_sums[0],
        early_sums[1],
    )


def solution(mesh):
    placed = (
        P("dp", "col", "row"),
        P("dp", "col", None),
        P("dp", None),
        P("dp", None),
        P("dp", "col", "row"),
        P("row"),
        P(),
        P("row", "col"),
        P(),
        P(),
        P("col", "row"),
        P("row"),
        P("row", "col"),
        P("col", "row"),
        P("row"),
        P("row", "col"),
        P("row", "col"),
        P("row", "col"),
        P("col", "row"),
        P("row"),
        P("row", "col"),
        P("col", "row"),
    )
    sizes = dict(mesh.shape)
    quick = sizes == {"row": 2, "col": 4, "dp": 4}
    return jax.shard_map(
        fast_device if quick else on_device,
        mesh=mesh,
        in_specs=placed,
        out_specs=(
            P("dp", "col", "row"),
            P("dp", "col", "row"),
            P("dp", "col", None),
            P("row"),
            P(),
            P("row", "col"),
            P(),
            P(),
            P("col", "row"),
            P("row"),
            P("row", "col"),
            P("col", "row"),
            P("row"),
            P("row", "col"),
            P("row", "col"),
            P("row", "col"),
            P("col", "row"),
            P("row"),
            P("row", "col"),
            P("col", "row"),
        ),
        check_vma=False,
    )
```
